32 devices in a mesh: grp: 4 (over x, core), slab: 8 (over z, y).
Axes of the slice: x: 2, y: 2, z: 4, core: 2. Of those that a mesh axis runs over, the one named last changes fastest.
Arguments:
- velocity: float32 [3, 8, 256, 256], P(None, 'slab', 'grp'), may hold values from -2.5 to 2.5
- fields: bfloat16 [8, 3, 8, 256, 256], P('grp', None, 'slab'), may hold values from -8 to 8
- noise: float32 [8, 3], P('grp'), may hold values from -4 to 4
Outputs:
- new_velocity: float32 [3, 8, 256, 256], P(None, 'slab', 'grp')
- new_fields: bfloat16 [8, 3, 8, 256, 256], P('grp', None, 'slab')
The draws below stay inside these ranges and needn't reach their ends.
All inputs are finite; a program needn't handle non-finite values.
Results may differ from the reference program's by a relative error of at most 0.0004.
Values may be sent and summed in bfloat16 or wider, within the bound.
No kernel may reach another device: no remote copies, remote signals or barrier semaphores. Data moves between devices by JAX's collectives and lax.ppermute only.
A program may use at most 64 MiB of HBM per device.

```python
import math
import jax
import jax.numpy as jnp
from jax import lax

NX = 256
NY = 256
NZ = 8
FIELDS = 8


def shard_levels(key, shape, pieces, low, largest):
    def one(dim, blocks):
        draws = jax.random.uniform(jax.random.fold_in(jax.random.fold_in(key, 6), dim), (blocks,), jnp.float32, low / len(pieces), largest / len(pieces))
        return jnp.repeat(jnp.exp(draws), shape[dim] // blocks).reshape((-1,) + (1,) * (len(shape) - dim - 1))

    gain = one(*pieces[0])
    for cut in pieces[1:]:
        gain = gain * one(*cut)
    return gain


def scatter_about(own_key, shape, spread, most, split=(), kind=jnp.bfloat16):
    values = jax.random.normal(own_key, shape, jnp.float32) * spread
    if len(split) > 0:
        values = shard_levels(own_key, shape, split, -0.22, 0.18) * values
    return jnp.clip(values, min=-most, max=most).astype(kind)


def setup_inputs(seed: int = 0) -> dict:
    keys = jax.random.split(jax.random.key(seed), 4)
    return {
        "velocity": scatter_about(keys[0], (3, NZ, NX, NY), 0.6, 2.5, ((1, 8), (2, 4)), jnp.float32),
        "fields": scatter_about(keys[1], (FIELDS, 3, NZ, NX, NY), 1.5, 8.0, ((0, 4), (2, 8))),
        "noise": scatter_about(keys[2], (FIELDS, 3), 1.0, 4.0, ((0, 4),), jnp.float32),
    }


TIME_STEP = 0.05
RELAX_TIME = 0.1
STRETCH_MAX = 36.0
POLY_MODULUS = 2.0
VISCOSITY = 0.2
NOISE_SCALE = math.sqrt(TIME_STEP / RELAX_TIME)
TENSOR_PAIRS = ((0, 0), (1, 1), (2, 2), (0, 1), (0, 2), (1, 2))

def pair_slot(first_axis, second_axis):
    return TENSOR_PAIRS.index((min(first_axis, second_axis), max(first_axis, second_axis)))

def centred(values, axis):
    return (jnp.roll(values, -1, axis) - jnp.roll(values, 1, axis)) * 0.5

def reference(velocity, fields, noise):
    directions = (1, 2, 0)
    gradient = jnp.stack([centred(velocity[component], directions[direction]) for component in range(3) for direction in range(3)])

    def add_field(total, member):
        conform = member.astype(jnp.float32)
        return (total + jnp.stack([conform[first] * conform[second] for first, second in TENSOR_PAIRS]), None)
    sums, unused = lax.scan(add_field, jnp.zeros((6, NZ, NX, NY), jnp.float32), fields)
    stretch = 1.0 / (1.0 - (sums[0] + sums[1] + sums[2]) / FIELDS / STRETCH_MAX)
    identity = jnp.array([1.0, 1.0, 1.0, 0.0, 0.0, 0.0], jnp.float32)[:, None, None, None]
    stress = POLY_MODULUS * (stretch * sums / FIELDS - identity)

    def advance(item):
        member, kick = item
        conform = member.astype(jnp.float32)
        updated = []
        for component in range(3):
            advect = sum((velocity[direction] * centred(conform[component], directions[direction]) for direction in range(3)))
            stretching = sum((gradient[3 * component + direction] * conform[direction] for direction in range(3)))
            drift = stretching - advect - stretch * conform[component] / (2.0 * RELAX_TIME)
            updated.append(conform[component] + TIME_STEP * drift + NOISE_SCALE * kick[component])
        return jnp.stack(updated).astype(jnp.bfloat16)
    new_fields = lax.map(advance, (fields, noise))
    forcing = []
    for component in range(3):
        convect = sum((velocity[direction] * gradient[3 * component + direction] for direction in range(3)))
        divergence = sum((centred(stress[pair_slot(component, direction)], directions[direction]) for direction in range(3)))
        forcing.append(velocity[component] + TIME_STEP * (divergence - convect))
    forcing = jnp.stack(forcing)
    spectrum = jnp.fft.fftn(forcing, axes=(1, 2, 3))
    wave_z = (jnp.fft.fftfreq(NZ) * (2.0 * math.pi))[:, None, None]
    wave_x = (jnp.fft.fftfreq(NX) * (2.0 * math.pi))[None, :, None]
    wave_y = (jnp.fft.fftfreq(NY) * (2.0 * math.pi))[None, None, :]
    waves = (wave_x, wave_y, wave_z)
    square = wave_x * wave_x + wave_y * wave_y + wave_z * wave_z
    safe_square = jnp.where(square > 0, square, 1.0)
    projected = (wave_x * spectrum[0] + wave_y * spectrum[1] + wave_z * spectrum[2]) / safe_square
    damping = 1.0 + VISCOSITY * TIME_STEP * square
    solved = jnp.stack([(spectrum[component] - waves[component] * projected) / damping for component in range(3)])
    new_velocity = jnp.fft.ifftn(solved, axes=(1, 2, 3)).real.astype(jnp.float32)
    return (new_velocity, new_fields)
```

```python
import math

import jax
import jax.numpy as jnp
import numpy as np
from jax import lax
from jax.experimental import pallas as pl
from jax.experimental.pallas import tpu as pltpu
from jax.sharding import PartitionSpec as P

TIME_STEP = 0.05
RELAX_TIME = 0.1
STRETCH_MAX = 36.0
POLY_MODULUS = 2.0
VISCOSITY = 0.2
NOISE_SCALE = math.sqrt(TIME_STEP / RELAX_TIME)
TENSOR_PAIRS = ((0, 0), (1, 1), (2, 2), (0, 1), (0, 2), (1, 2))


def extended(block, sides, width):
    for axis, dim in sides:
        count = lax.axis_size(axis)
        forward = [(i, i + 1) for i in range(count - 1)]
        forward.append((count - 1, 0))
        backward = [(target, source) for source, target in forward]
        low = lax.ppermute(
            lax.slice_in_dim(block, block.shape[dim] - width, None, axis=dim), axis, forward
        )
        high = lax.ppermute(lax.slice_in_dim(block, 0, width, axis=dim), axis, backward)
        block = jnp.concatenate([low, block, high], axis=dim)
    return block


def pair_slot(first_axis, second_axis):
    return TENSOR_PAIRS.index((min(first_axis, second_axis), max(first_axis, second_axis)))


def centred(values, axis):
    return (jnp.roll(values, -1, axis) - jnp.roll(values, 1, axis)) * 0.5


def stack_gradient(parts):
    return jnp.stack(
        [parts[direction][component] for component in range(3) for direction in range(3)]
    )


def pair_products(conform):
    return jnp.stack(
        [jnp.sum(conform[:, first] * conform[:, second], axis=0) for first, second in TENSOR_PAIRS]
    )


def stretch_factor(mean_square):
    return 1.0 / (1.0 - mean_square / STRETCH_MAX)


def poly_stress(sums, stretch, field_total):
    identity = jnp.array([1.0, 1.0, 1.0, 0.0, 0.0, 0.0], jnp.float32)[:, None, None, None]
    return POLY_MODULUS * (stretch * sums / field_total - identity)


def dft_tables(length):
    counter = jnp.arange(length, dtype=jnp.int32)
    phase = counter[:, None] * counter[None, :] % length
    angle = phase.astype(jnp.float32) * (2.0 * math.pi / length)
    return (jnp.cos(angle), jnp.sin(angle))


def along_axis(values, table, axis):
    letters = "abcdef"[: values.ndim]
    result = letters[:axis] + "k" + letters[axis + 1 :]
    return jnp.einsum(
        letters + "," + letters[axis] + "k->" + result,
        values,
        table,
        precision=lax.Precision.HIGHEST,
    )


def complex_pass(stacked, axis, forward):
    cosine, sine_table = dft_tables(stacked.shape[axis])
    cos_terms = along_axis(stacked, cosine, axis)
    sin_terms = along_axis(stacked, sine_table, axis)
    if forward:
        return jnp.stack([cos_terms[0] + sin_terms[1], cos_terms[1] - sin_terms[0]])
    return jnp.stack([cos_terms[0] - sin_terms[1], cos_terms[1] + sin_terms[0]])


def wavenumber(indices, length):
    signed = jnp.where(indices < length // 2, indices, indices - length)
    return signed.astype(jnp.float32) * (2.0 * math.pi / length)


def shards(velocity, fields, noise):
    grp_count = lax.axis_size("grp")
    grp_index = lax.axis_index("grp")
    slab_count = lax.axis_size("slab")
    slab_index = lax.axis_index("slab")
    field_total = fields.shape[0] * grp_count
    row_count = velocity.shape[2]
    row_start = grp_index * row_count
    width_y = velocity.shape[3]
    rimmed = extended(velocity, (("grp", 2), ("slab", 1)), 1)
    along_x = (rimmed[:, 1:-1, 2:, :] - rimmed[:, 1:-1, :-2, :]) * 0.5
    along_y = centred(velocity, 3)
    along_z = (rimmed[:, 2:, 1:-1, :] - rimmed[:, :-2, 1:-1, :]) * 0.5
    grad_rows = stack_gradient((along_x, along_y, along_z))
    grad_plane, vel_plane = (
        lax.all_gather(grad_rows, "grp", axis=2, tiled=True),
        lax.all_gather(velocity, "grp", axis=2, tiled=True),
    )
    field_rim = extended(fields, (("slab", 2),), 1)
    conform = fields.astype(jnp.float32)
    field_dz = (
        field_rim[:, :, 2:].astype(jnp.float32) - field_rim[:, :, :-2].astype(jnp.float32)
    ) * 0.5
    summed = lax.psum(pair_products(conform), "grp")
    stretch = stretch_factor((summed[0] + summed[1] + summed[2]) / field_total)
    stress_plane = poly_stress(summed, stretch, field_total)
    wrapped = jnp.concatenate(
        [stress_plane[:, :, -1:], stress_plane, stress_plane[:, :, :1]], axis=2
    )
    stress_rows = lax.dynamic_slice_in_dim(wrapped, row_start, row_count + 2, 2)
    stress_pad = extended(stress_rows, (("slab", 1),), 1)
    updated = []
    for component in range(3):
        member = conform[:, component]
        advect = (
            vel_plane[0] * centred(member, 2)
            + vel_plane[1] * centred(member, 3)
            + vel_plane[2] * field_dz[:, component]
        )
        stretching = sum(
            (
                grad_plane[3 * component + direction] * conform[:, direction]
                for direction in range(3)
            )
        )
        drift = stretching - advect - stretch * member / (2.0 * RELAX_TIME)
        updated.append(
            member + TIME_STEP * drift + NOISE_SCALE * noise[:, component][:, None, None, None]
        )
    new_fields = jnp.stack(updated, axis=1).astype(jnp.bfloat16)
    forcing = []
    for component in range(3):
        convect = sum(
            (velocity[direction] * grad_rows[3 * component + direction] for direction in range(3))
        )
        slot_x = pair_slot(component, 0)
        slot_y = pair_slot(component, 1)
        slot_z = pair_slot(component, 2)
        divergence = (stress_pad[slot_x, 1:-1, 2:, :] - stress_pad[slot_x, 1:-1, :-2, :]) * 0.5
        divergence = divergence + centred(stress_pad[slot_y, 1:-1, 1:-1, :], 2)
        divergence = (
            divergence + (stress_pad[slot_z, 2:, 1:-1, :] - stress_pad[slot_z, :-2, 1:-1, :]) * 0.5
        )
        forcing.append(velocity[component] + TIME_STEP * (divergence - convect))
    forcing = jnp.stack(forcing)
    cosine_y, sine_y = dft_tables(width_y)
    flat = forcing.reshape(-1, width_y)
    real_part = jnp.dot(flat, cosine_y, precision=lax.Precision.HIGHEST).reshape(forcing.shape)
    imag_part = -jnp.dot(flat, sine_y, precision=lax.Precision.HIGHEST).reshape(forcing.shape)
    spectrum = jnp.stack([real_part, imag_part])
    spectrum = lax.all_to_all(spectrum, "grp", split_axis=4, concat_axis=3, tiled=True)
    spectrum = complex_pass(spectrum, 3, True)
    spectrum = lax.all_to_all(spectrum, "slab", split_axis=3, concat_axis=2, tiled=True)
    spectrum = complex_pass(spectrum, 2, True)
    total_z = spectrum.shape[2]
    cols_x = spectrum.shape[3]
    cols_y = spectrum.shape[4]
    total_x = cols_x * slab_count
    total_y = cols_y * grp_count
    wave_z = wavenumber(jnp.arange(total_z, dtype=jnp.int32), total_z)[:, None, None]
    wave_x = wavenumber(slab_index * cols_x + jnp.arange(cols_x, dtype=jnp.int32), total_x)[
        None, :, None
    ]
    wave_y = wavenumber(grp_index * cols_y + jnp.arange(cols_y, dtype=jnp.int32), total_y)[
        None, None, :
    ]
    waves = (wave_x, wave_y, wave_z)
    square = wave_x * wave_x + wave_y * wave_y + wave_z * wave_z
    safe_square = jnp.where(square > 0, square, 1.0)
    projected = (
        wave_x * spectrum[:, 0] + wave_y * spectrum[:, 1] + wave_z * spectrum[:, 2]
    ) / safe_square
    damping = 1.0 + VISCOSITY * TIME_STEP * square
    solved = jnp.stack(
        [
            (spectrum[:, component] - waves[component] * projected) / damping
            for component in range(3)
        ],
        axis=1,
    )
    solved = complex_pass(solved, 2, False)
    solved = lax.all_to_all(solved, "slab", split_axis=2, concat_axis=3, tiled=True)
    solved = complex_pass(solved, 3, False)
    solved = lax.all_to_all(solved, "grp", split_axis=3, concat_axis=4, tiled=True)
    flat_real = solved[0].reshape(-1, width_y)
    flat_imag = solved[1].reshape(-1, width_y)
    combined = jnp.dot(flat_real, cosine_y, precision=lax.Precision.HIGHEST) - jnp.dot(
        flat_imag, sine_y, precision=lax.Precision.HIGHEST
    )
    new_velocity = combined.reshape(velocity.shape) / (width_y * total_x * total_z)
    return (new_velocity, new_fields)


ROW_TILE = 16


def real_basis(length):
    half = length // 2
    cell = np.arange(length)
    wave = np.arange(half)
    angle = (cell[:, None] * wave[None, :] % length) * (2.0 * math.pi / length)
    sine = np.sin(angle)
    sine[:, 0] = np.where(cell % 2 == 0, 1.0, -1.0)
    return np.concatenate([np.cos(angle), sine], axis=1)


def split_table(table):
    high = jnp.asarray(table.astype(jnp.bfloat16))
    low = jnp.asarray((table - table.astype(jnp.bfloat16).astype(np.float64)).astype(jnp.bfloat16))
    return high, low


def split_value(value):
    high = value.astype(jnp.bfloat16)
    return high, (value - high.astype(jnp.float32)).astype(jnp.bfloat16)


def dot_split(left, right, dims):
    def one(a, b):
        return lax.dot_general(a, b, (dims, ((), ())), preferred_element_type=jnp.float32)

    return one(left[0], right[0]) + (one(left[0], right[1]) + one(left[1], right[0]))


def row_index(shape):
    return lax.broadcasted_iota(jnp.int32, shape, 0)


def lane_index(shape):
    return lax.broadcasted_iota(jnp.int32, shape, 1)


def row_after(block, last):
    rows = block.shape[0]
    moved = pltpu.roll(block, rows - 1, 0)
    return jnp.where(row_index(block.shape) == rows - 1, last, moved)


def row_before(block, first):
    moved = pltpu.roll(block, 1, 0)
    return jnp.where(row_index(block.shape) == 0, first, moved)


def lane_difference(block):
    lanes = block.shape[1]
    return pltpu.roll(block, lanes - 1, 1) - pltpu.roll(block, 1, 1)


def whole(array):
    rank = len(array.shape)
    return pl.BlockSpec(array.shape, lambda *_: (0,) * rank)


def run_kernel(body, outs, args, scalars=(), scratch=(), cost=None):
    in_specs = [pl.BlockSpec(memory_space=pltpu.SMEM) for _ in scalars]
    in_specs += [whole(a) for a in args]
    return pl.pallas_call(
        body,
        out_shape=outs,
        grid=(1,),
        in_specs=in_specs,
        out_specs=jax.tree.map(whole, outs),
        scratch_shapes=scratch,
        cost_estimate=cost,
        name=body.__name__ if hasattr(body, "__name__") else None,
    )(*scalars, *args)


def pack_rows(fields, grp_index, groups):
    members, dims, size_x, size_y = fields.shape
    rows = size_x // groups
    planes = members * dims
    rim = -(-2 * planes // ROW_TILE) * ROW_TILE
    shape = jax.ShapeDtypeStruct((planes * rows + rim, size_y), fields.dtype)

    def pack(index, source, *targets):
        for shift, target in enumerate(targets):
            block = (index[0] + shift) % groups
            start = pl.multiple_of(block * rows, rows)
            above = pl.multiple_of((block + groups - 1) % groups * rows + rows - ROW_TILE, ROW_TILE)
            below = pl.multiple_of((block + 1) % groups * rows, rows)
            edge = jnp.zeros((rim, size_y), jnp.float32)
            place = row_index((rim, size_y))
            for member in range(members):
                for dim in range(dims):
                    plane = member * dims + dim
                    target[plane * rows : (plane + 1) * rows, :] = source[
                        member, dim, pl.ds(start, rows), :
                    ]
                    top = source[member, dim, pl.ds(above, ROW_TILE), :].astype(jnp.float32)
                    bottom = source[member, dim, pl.ds(below, ROW_TILE), :].astype(jnp.float32)
                    slot = dim * 2 * members + member * 2
                    edge = jnp.where(place == slot, top[ROW_TILE - 1 :], edge)
                    edge = jnp.where(place == slot + 1, bottom[:1], edge)
            target[planes * rows :, :] = edge.astype(fields.dtype)

    return run_kernel(pack, [shape] * groups, [fields], [grp_index])


def force_rows(blocks, motion, above, below, table, members, field_total):
    rows, size_y = motion.shape[1:]
    planes = 3 * members

    def stress_of(sums):
        stretch = stretch_factor((sums[0] + sums[1] + sums[2]) / field_total)
        return stretch, [
            POLY_MODULUS * (stretch * sums[slot] / field_total - (1.0 if first == second else 0.0))
            for slot, (first, second) in enumerate(TENSOR_PAIRS)
        ]

    def force(*refs):
        parts = refs[: len(blocks)]
        flow, top, bottom, table_high, table_low, out, stretch_out, stress, stack = refs[
            len(blocks) :
        ]
        for start in range(0, rows, ROW_TILE):
            sums = [None] * 6
            for part in parts:
                for member in range(members):
                    vector = [
                        part[
                            (member * 3 + dim) * rows + start : (member * 3 + dim) * rows
                            + start
                            + ROW_TILE,
                            :,
                        ].astype(jnp.float32)
                        for dim in range(3)
                    ]
                    for slot, (first, second) in enumerate(TENSOR_PAIRS):
                        term = vector[first] * vector[second]
                        sums[slot] = term if sums[slot] is None else sums[slot] + term
            stretch, values = stress_of(sums)
            stretch_out[start : start + ROW_TILE, :] = stretch
            for slot in range(6):
                stress[slot, start : start + ROW_TILE, :] = values[slot]
        sums = [None] * 6
        for part in parts:
            edge = part[planes * rows :, :].astype(jnp.float32)
            vector = [edge[dim * 2 * members : (dim + 1) * 2 * members] for dim in range(3)]
            for slot, (first, second) in enumerate(TENSOR_PAIRS):
                term = vector[first] * vector[second]
                sums[slot] = term if sums[slot] is None else sums[slot] + term
        sums = [
            sum(value[2 * member : 2 * member + 2] for member in range(members)) for value in sums
        ]
        edges = stress_of(sums)[1]
        half = 0.5 * TIME_STEP
        place = {0: 0, 1: 1, 2: 4}
        for component in range(3):
            slot_x = pair_slot(component, 0)
            slot_y = pair_slot(component, 1)
            slot_z = pair_slot(component, 2)
            value = stress[slot_x]
            total = row_after(value, edges[slot_x][1:2]) - row_before(value, edges[slot_x][0:1])
            total = total + lane_difference(stress[slot_y])
            own = flow[component]
            total = total - flow[0] * (
                row_after(own, bottom[component]) - row_before(own, top[component])
            )
            total = total - flow[1] * lane_difference(own)
            total = total - (2.0 * flow[2]) * flow[3 + component]
            spot = place[component]
            stack[spot * rows : (spot + 1) * rows, :] = own + half * total
            spot = spot + (2 if component < 2 else 1)
            stack[spot * rows : (spot + 1) * rows, :] = half * stress[slot_z]
        out[...] = dot_split(
            (table_high[...], table_low[...]), split_value(stack[...]), ((1,), (1,))
        )

    return run_kernel(
        force,
        [
            jax.ShapeDtypeStruct((size_y, 6 * rows), jnp.float32),
            jax.ShapeDtypeStruct((rows, size_y), jnp.float32),
        ],
        [*blocks, motion, above, below, *table],
        scratch=[
            pltpu.VMEM((6, rows, size_y), jnp.float32),
            pltpu.VMEM((6 * rows, size_y), jnp.float32),
        ],
    )


def solve_pencil(pencil, device_index, table, groups, total_z, size_y):
    block = pencil.shape[1]
    pairs = block // 2
    rows = pencil.shape[2] // 6
    size_x = rows * groups
    half_x = size_x // 2
    half_z = total_z // 2
    basis_z = real_basis(total_z)
    lines = total_z * block
    step_x = 2.0 * math.pi / size_x
    step_y = 2.0 * math.pi / size_y
    step_z = 2.0 * math.pi / total_z

    def join(first, second, lane):
        return jnp.where(lane < rows, first, pltpu.roll(second, rows, 1))

    def solve(index, source, table_high, table_low, out, stack, result):
        lane = lane_index((block, 2 * rows))
        for pair in range(groups // 2):
            both = []
            for side in range(2):
                group = 2 * pair + side
                tiles = [
                    [
                        source[group * total_z + z, :, t * 2 * rows : (t + 1) * 2 * rows]
                        for t in range(3)
                    ]
                    for z in range(total_z)
                ]
                both.append(
                    [
                        (
                            tiles[z][0] + tiles[(z + 1) % total_z][1] - tiles[z - 1][1],
                            tiles[z][2]
                            + pltpu.roll(tiles[(z + 1) % total_z][2] - tiles[z - 1][2], rows, 1),
                        )
                        for z in range(total_z)
                    ]
                )
            columns = slice(pair * 2 * rows, (pair + 1) * 2 * rows)
            for z in range(total_z):
                (first, third), (first_b, third_b) = both[0][z], both[1][z]
                line = z * block
                stack[line : line + block, columns] = join(first, first_b, lane)
                stack[lines + line : lines + line + block, columns] = jnp.where(
                    lane < rows, pltpu.roll(first, rows, 1), first_b
                )
                stack[2 * lines + line : 2 * lines + line + block, columns] = join(
                    third, third_b, lane
                )
        table_x = (table_high[...], table_low[...])
        result[...] = dot_split(split_value(stack[...]), table_x, ((1,), (0,)))

        shape = (block, size_x)
        lane = lane_index(shape)
        row = row_index(shape)
        wave = (lane % half_x).astype(jnp.float32) * step_x
        nyquist_x = jnp.where(lane == half_x, math.pi, 0.0)
        swap_x = jnp.where(lane < half_x, wave, -wave)
        square_x = wave * wave + nyquist_x * nyquist_x
        weight_x = jnp.where(lane % half_x == 0, 1.0, 2.0)
        number = index[0] * pairs + row % pairs
        wave = number.astype(jnp.float32) * step_y
        nyquist_y = jnp.where((number == 0) & (row >= pairs), math.pi, 0.0)
        swap_y = jnp.where(row < pairs, wave, -wave)
        square_y = wave * wave + nyquist_y * nyquist_y
        weight_y = jnp.where(number == 0, 1.0, 2.0)
        square_xy = square_x + square_y
        scale = weight_x * weight_y / (size_x * size_y * total_z)

        def along_x(value):
            return swap_x * pltpu.roll(value, half_x, 1)

        def along_y(value):
            return swap_y * pltpu.roll(value, pairs, 0)

        waves = []
        for component in range(3):
            planes = [
                result[component * lines + z * block : component * lines + (z + 1) * block, :]
                for z in range(total_z)
            ]
            waves.append(
                [
                    sum(float(basis_z[z, k]) * planes[z] for z in range(total_z))
                    for k in range(total_z)
                ]
            )

        def partner(k):
            if k % half_z == 0:
                return k, 0.0
            return (k + half_z, step_z * k) if k < half_z else (k - half_z, -step_z * (k - half_z))

        potential = []
        factors = []
        extra = []
        for k in range(total_z):
            wave_z = step_z * (k % half_z) if k != half_z else math.pi
            square = square_xy + wave_z * wave_z
            safe = jnp.where(square > 0, square, 1.0)
            other, factor = partner(k)
            total = along_x(waves[0][k]) + along_y(waves[1][k])
            if factor != 0.0:
                total = total + factor * waves[2][other]
            potential.append(total / safe)
            nyquist = nyquist_x * waves[0][k] + nyquist_y * waves[1][k]
            if k == half_z:
                nyquist = nyquist + math.pi * waves[2][k]
            extra.append(nyquist / safe)
            weight_z = 1.0 if k % half_z == 0 else 2.0
            factors.append(scale * weight_z / (1.0 + VISCOSITY * TIME_STEP * square))
        solved = [[], [], []]
        for k in range(total_z):
            other, factor = partner(k)
            solved[0].append(
                factors[k] * (waves[0][k] + along_x(potential[k]) - nyquist_x * extra[k])
            )
            solved[1].append(
                factors[k] * (waves[1][k] + along_y(potential[k]) - nyquist_y * extra[k])
            )
            value = waves[2][k]
            if factor != 0.0:
                value = value + factor * potential[other]
            if k == half_z:
                value = value - math.pi * extra[k]
            solved[2].append(factors[k] * value)
        for component in range(3):
            for z in range(total_z):
                line = component * lines + z * block
                stack[line : line + block, :] = sum(
                    float(basis_z[z, k]) * solved[component][k] for k in range(total_z)
                )
        result[...] = dot_split(split_value(stack[...]), table_x, ((1,), (1,)))
        lane = lane_index((block, 2 * rows))
        for group in range(groups):
            columns = slice(group // 2 * 2 * rows, (group // 2 + 1) * 2 * rows)
            for z in range(total_z):
                line = z * block
                first, second, third = [
                    result[c * lines + line : c * lines + line + block, columns] for c in range(3)
                ]
                if group % 2 == 0:
                    front = join(first, second, lane)
                else:
                    front = jnp.where(lane < rows, pltpu.roll(first, rows, 1), second)
                    third = pltpu.roll(third, rows, 1)
                out[group * total_z + z, :, : 2 * rows] = front
                out[group * total_z + z, :, 2 * rows :] = third

    return run_kernel(
        solve,
        jax.ShapeDtypeStruct((groups * total_z, block, 4 * rows), jnp.float32),
        [pencil, *table],
        [device_index],
        scratch=[
            pltpu.VMEM((3 * lines, size_x), jnp.float32),
            pltpu.VMEM((3 * lines, size_x), jnp.float32),
        ],
    )


def rows_from_waves(spectra, table, rows):
    size_y = table[0].shape[1]

    def synthesise(source, table_high, table_low, out):
        turned = source[...].T[: 3 * rows]
        value = dot_split(
            split_value(turned), (table_high[...], table_low[...]), ((1,), (0,))
        )
        for component in range(3):
            out[component, 0] = value[component * rows : (component + 1) * rows]

    return run_kernel(
        synthesise,
        jax.ShapeDtypeStruct((3, 1, rows, size_y), jnp.float32),
        [spectra, *table],
    )


def advance_fields(fields, paired, passed, motions, stretches, noise, spots, sign):
    members, dims, size_x, size_y = fields.shape
    count = len(motions)
    rows = size_x // count
    steps = size_x // ROW_TILE

    def advance(spot, signs, kick, *refs):
        own, near, far = refs[:3]
        flows = refs[3 : 3 + count]
        factors = refs[3 + count : 3 + 2 * count]
        out, plane, factor = refs[3 + 2 * count :]
        for number in range(count):
            start = pl.multiple_of(spot[number] * rows, rows)
            for slot in range(6):
                plane[slot, pl.ds(start, rows), :] = flows[number][slot]
            factor[pl.ds(start, rows), :] = factors[number][...]
        side = signs[0].astype(jnp.float32)
        half = 0.5 * TIME_STEP

        def step(number, carry):
            start = pl.multiple_of(number * ROW_TILE, ROW_TILE)
            before = pl.multiple_of((number + steps - 1) % steps * ROW_TILE, ROW_TILE)
            after = pl.multiple_of((number + 1) % steps * ROW_TILE, ROW_TILE)
            here = pl.ds(start, ROW_TILE)
            speed = [half * plane[c, here, :] for c in range(3)]
            slope = []
            for c in range(3):
                first = half * plane[c, pl.ds(before, ROW_TILE), :][ROW_TILE - 1 :]
                last = half * plane[c, pl.ds(after, ROW_TILE), :][:1]
                slope.append(
                    (
                        row_after(speed[c], last) - row_before(speed[c], first),
                        lane_difference(speed[c]),
                        TIME_STEP * plane[3 + c, here, :],
                    )
                )
            keep = 1.0 - (TIME_STEP / (2.0 * RELAX_TIME)) * factor[here, :]
            lift = side * speed[2]
            for member in range(members):
                vector = [own[member, c, here, :].astype(jnp.float32) for c in range(3)]
                for c in range(3):
                    first = own[member, c, pl.ds(before, ROW_TILE), :].astype(jnp.float32)
                    last = own[member, c, pl.ds(after, ROW_TILE), :].astype(jnp.float32)
                    value = vector[c]
                    rise = near[member, c, here, :].astype(jnp.float32) - far[
                        member, c, here, :
                    ].astype(jnp.float32)
                    total = keep * value + NOISE_SCALE * kick[member, c]
                    for j in range(3):
                        total = total + slope[c][j] * vector[j]
                    total = total - speed[0] * (
                        row_after(value, last[:1]) - row_before(value, first[ROW_TILE - 1 :])
                    )
                    total = total - speed[1] * lane_difference(value)
                    total = total - lift * rise
                    out[member, c, here, :] = total.astype(jnp.bfloat16)
            return carry

        lax.fori_loop(0, steps, step, 0)

    return run_kernel(
        advance,
        jax.ShapeDtypeStruct(fields.shape, jnp.bfloat16),
        [fields, paired, passed, *motions, *stretches],
        [spots, sign, noise],
        scratch=[
            pltpu.VMEM((6, size_x, size_y), jnp.float32),
            pltpu.VMEM((size_x, size_y), jnp.float32),
        ],
        cost=pl.CostEstimate(flops=60000000, bytes_accessed=5000000, transcendentals=0),
    )


def shifted(value, axis, step):
    count = lax.axis_size(axis)
    return lax.ppermute(value, axis, [(i, (i + step) % count) for i in range(count)])


def flipped(value, axis, bit):
    count = lax.axis_size(axis)
    return lax.ppermute(value, axis, [(i, i ^ bit) for i in range(count)])


def spread(value, axis):
    bit = lax.axis_size(axis) // 2
    found = [(0, value)]
    while bit:
        found += [(offset ^ bit, flipped(held, axis, bit)) for offset, held in found]
        bit //= 2
    return found


def pencil_shards(velocity, fields, noise):
    groups = lax.axis_size("grp")
    slabs = lax.axis_size("slab")
    grp_index = lax.axis_index("grp")
    slab_index = lax.axis_index("slab")
    members, dims, _, size_x, size_y = fields.shape
    rows = velocity.shape[2]
    devices = groups * slabs
    block = size_y // devices
    half_block = block // 2
    order = np.concatenate(
        [
            np.concatenate([np.arange(half_block), size_y // 2 + np.arange(half_block)])
            + device * half_block
            for device in range(devices)
        ]
    )
    table_y = split_table(np.ascontiguousarray(real_basis(size_y).T[order]))
    table_x = split_table(real_basis(size_x))

    flow = velocity[:, 0]
    above = shifted(flow[:, -1:], "grp", 1)
    below = shifted(flow[:, :1], "grp", -1)
    lower = shifted(flow, "slab", 1)
    upper = shifted(flow, "slab", -1)
    plane = fields[:, :, 0]
    blocks = pack_rows(plane, grp_index.reshape(1), groups)
    blocks = [blocks[0]] + [shifted(blocks[d], "grp", d) for d in range(1, groups)]
    paired = flipped(plane, "slab", 1)
    passed = lax.ppermute(
        paired, "slab", [(i, (i + (-2 if i % 2 else 2)) % slabs) for i in range(slabs)]
    )
    motion = jnp.concatenate([flow, (upper - lower) * 0.5], axis=0)
    motions = spread(motion, "grp")
    spectra, stretch = force_rows(
        blocks, motion, above, below, table_y, members, members * groups
    )
    stretches = spread(stretch, "grp")
    pencil = lax.all_to_all(
        spectra.reshape(devices, block, 6 * rows),
        ("grp", "slab"),
        split_axis=0,
        concat_axis=0,
        tiled=True,
    )
    device_index = (grp_index * slabs + slab_index).reshape(1)
    solved = solve_pencil(pencil, device_index, table_x, groups, slabs, size_y)
    spots = jnp.stack([grp_index ^ offset for offset, _ in motions])
    sign = (1 - 2 * (slab_index % 2)).reshape(1)
    new_fields = advance_fields(
        plane,
        paired,
        passed,
        [held for _, held in motions],
        [held for _, held in stretches],
        noise,
        spots,
        sign,
    )
    solved = lax.all_to_all(
        solved, ("grp", "slab"), split_axis=0, concat_axis=0, tiled=True
    )
    new_velocity = rows_from_waves(solved.reshape(size_y, 4 * rows), table_y, rows)
    return (new_velocity, new_fields[:, :, None])


def pencil_fits(mesh, velocity, fields):
    groups, slabs = mesh.shape["grp"], mesh.shape["slab"]
    size_z, size_x, size_y = velocity.shape[1:]
    return (
        size_z == slabs
        and slabs % 2 == 0
        and groups >= 2
        and groups & (groups - 1) == 0
        and size_y % (2 * groups * slabs) == 0
        and size_x % (groups * ROW_TILE) == 0
        and (2 * size_x // groups) % 128 == 0
        and fields.shape[0] % groups == 0
    )


def solution(mesh):
    def step(velocity, fields, noise):
        body = pencil_shards if pencil_fits(mesh, velocity, fields) else shards
        return jax.shard_map(
            body,
            mesh=mesh,
            in_specs=(
                P(None, "slab", "grp", None),
                P("grp", None, "slab", None, None),
                P("grp", None),
            ),
            out_specs=(P(None, "slab", "grp", None), P("grp", None, "slab", None, None)),
            check_vma=False,
        )(velocity, fields, noise)

    return step
```

```python
import math

import jax
import jax.numpy as jnp
import numpy as np
from jax import lax
from jax.experimental import pallas as pl
from jax.experimental.pallas import tpu as pltpu
from jax.sharding import PartitionSpec as P

TIME_STEP = 0.05
RELAX_TIME = 0.1
STRETCH_MAX = 36.0
POLY_MODULUS = 2.0
VISCOSITY = 0.2
NOISE_SCALE = math.sqrt(TIME_STEP / RELAX_TIME)
TENSOR_PAIRS = ((0, 0), (1, 1), (2, 2), (0, 1), (0, 2), (1, 2))


def extended(block, sides, width):
    for axis, dim in sides:
        count = lax.axis_size(axis)
        forward = [(i, i + 1) for i in range(count - 1)]
        forward.append((count - 1, 0))
        backward = [(target, source) for source, target in forward]
        low = lax.ppermute(
            lax.slice_in_dim(block, block.shape[dim] - width, None, axis=dim), axis, forward
        )
        high = lax.ppermute(lax.slice_in_dim(block, 0, width, axis=dim), axis, backward)
        block = jnp.concatenate([low, block, high], axis=dim)
    return block


def pair_slot(first_axis, second_axis):
    return TENSOR_PAIRS.index((min(first_axis, second_axis), max(first_axis, second_axis)))


def centred(values, axis):
    return (jnp.roll(values, -1, axis) - jnp.roll(values, 1, axis)) * 0.5


def stack_gradient(parts):
    return jnp.stack(
        [parts[direction][component] for component in range(3) for direction in range(3)]
    )


def pair_products(conform):
    return jnp.stack(
        [jnp.sum(conform[:, first] * conform[:, second], axis=0) for first, second in TENSOR_PAIRS]
    )


def stretch_factor(mean_square):
    return 1.0 / (1.0 - mean_square / STRETCH_MAX)


def poly_stress(sums, stretch, field_total):
    identity = jnp.array([1.0, 1.0, 1.0, 0.0, 0.0, 0.0], jnp.float32)[:, None, None, None]
    return POLY_MODULUS * (stretch * sums / field_total - identity)


def dft_tables(length):
    counter = jnp.arange(length, dtype=jnp.int32)
    phase = counter[:, None] * counter[None, :] % length
    angle = phase.astype(jnp.float32) * (2.0 * math.pi / length)
    return (jnp.cos(angle), jnp.sin(angle))


def along_axis(values, table, axis):
    letters = "abcdef"[: values.ndim]
    result = letters[:axis] + "k" + letters[axis + 1 :]
    return jnp.einsum(
        letters + "," + letters[axis] + "k->" + result,
        values,
        table,
        precision=lax.Precision.HIGHEST,
    )


def complex_pass(stacked, axis, forward):
    cosine, sine_table = dft_tables(stacked.shape[axis])
    cos_terms = along_axis(stacked, cosine, axis)
    sin_terms = along_axis(stacked, sine_table, axis)
    if forward:
        return jnp.stack([cos_terms[0] + sin_terms[1], cos_terms[1] - sin_terms[0]])
    return jnp.stack([cos_terms[0] - sin_terms[1], cos_terms[1] + sin_terms[0]])


def wavenumber(indices, length):
    signed = jnp.where(indices < length // 2, indices, indices - length)
    return signed.astype(jnp.float32) * (2.0 * math.pi / length)


def shards(velocity, fields, noise):
    grp_count = lax.axis_size("grp")
    grp_index = lax.axis_index("grp")
    slab_count = lax.axis_size("slab")
    slab_index = lax.axis_index("slab")
    field_total = fields.shape[0] * grp_count
    row_count = velocity.shape[2]
    row_start = grp_index * row_count
    width_y = velocity.shape[3]
    rimmed = extended(velocity, (("grp", 2), ("slab", 1)), 1)
    along_x = (rimmed[:, 1:-1, 2:, :] - rimmed[:, 1:-1, :-2, :]) * 0.5
    along_y = centred(velocity, 3)
    along_z = (rimmed[:, 2:, 1:-1, :] - rimmed[:, :-2, 1:-1, :]) * 0.5
    grad_rows = stack_gradient((along_x, along_y, along_z))
    grad_plane, vel_plane = (
        lax.all_gather(grad_rows, "grp", axis=2, tiled=True),
        lax.all_gather(velocity, "grp", axis=2, tiled=True),
    )
    field_rim = extended(fields, (("slab", 2),), 1)
    conform = fields.astype(jnp.float32)
    field_dz = (
        field_rim[:, :, 2:].astype(jnp.float32) - field_rim[:, :, :-2].astype(jnp.float32)
    ) * 0.5
    summed = lax.psum(pair_products(conform), "grp")
    stretch = stretch_factor((summed[0] + summed[1] + summed[2]) / field_total)
    stress_plane = poly_stress(summed, stretch, field_total)
    wrapped = jnp.concatenate(
        [stress_plane[:, :, -1:], stress_plane, stress_plane[:, :, :1]], axis=2
    )
    stress_rows = lax.dynamic_slice_in_dim(wrapped, row_start, row_count + 2, 2)
    stress_pad = extended(stress_rows, (("slab", 1),), 1)
    updated = []
    for component in range(3):
        member = conform[:, component]
        advect = (
            vel_plane[0] * centred(member, 2)
            + vel_plane[1] * centred(member, 3)
            + vel_plane[2] * field_dz[:, component]
        )
        stretching = sum(
            (
                grad_plane[3 * component + direction] * conform[:, direction]
                for direction in range(3)
            )
        )
        drift = stretching - advect - stretch * member / (2.0 * RELAX_TIME)
        updated.append(
            member + TIME_STEP * drift + NOISE_SCALE * noise[:, component][:, None, None, None]
        )
    new_fields = jnp.stack(updated, axis=1).astype(jnp.bfloat16)
    forcing = []
    for component in range(3):
        convect = sum(
            (velocity[direction] * grad_rows[3 * component + direction] for direction in range(3))
        )
        slot_x = pair_slot(component, 0)
        slot_y = pair_slot(component, 1)
        slot_z = pair_slot(component, 2)
        divergence = (stress_pad[slot_x, 1:-1, 2:, :] - stress_pad[slot_x, 1:-1, :-2, :]) * 0.5
        divergence = divergence + centred(stress_pad[slot_y, 1:-1, 1:-1, :], 2)
        divergence = (
            divergence + (stress_pad[slot_z, 2:, 1:-1, :] - stress_pad[slot_z, :-2, 1:-1, :]) * 0.5
        )
        forcing.append(velocity[component] + TIME_STEP * (divergence - convect))
    forcing = jnp.stack(forcing)
    cosine_y, sine_y = dft_tables(width_y)
    flat = forcing.reshape(-1, width_y)
    real_part = jnp.dot(flat, cosine_y, precision=lax.Precision.HIGHEST).reshape(forcing.shape)
    imag_part = -jnp.dot(flat, sine_y, precision=lax.Precision.HIGHEST).reshape(forcing.shape)
    spectrum = jnp.stack([real_part, imag_part])
    spectrum = lax.all_to_all(spectrum, "grp", split_axis=4, concat_axis=3, tiled=True)
    spectrum = complex_pass(spectrum, 3, True)
    spectrum = lax.all_to_all(spectrum, "slab", split_axis=3, concat_axis=2, tiled=True)
    spectrum = complex_pass(spectrum, 2, True)
    total_z = spectrum.shape[2]
    cols_x = spectrum.shape[3]
    cols_y = spectrum.shape[4]
    total_x = cols_x * slab_count
    total_y = cols_y * grp_count
    wave_z = wavenumber(jnp.arange(total_z, dtype=jnp.int32), total_z)[:, None, None]
    wave_x = wavenumber(slab_index * cols_x + jnp.arange(cols_x, dtype=jnp.int32), total_x)[
        None, :, None
    ]
    wave_y = wavenumber(grp_index * cols_y + jnp.arange(cols_y, dtype=jnp.int32), total_y)[
        None, None, :
    ]
    waves = (wave_x, wave_y, wave_z)
    square = wave_x * wave_x + wave_y * wave_y + wave_z * wave_z
    safe_square = jnp.where(square > 0, square, 1.0)
    projected = (
        wave_x * spectrum[:, 0] + wave_y * spectrum[:, 1] + wave_z * spectrum[:, 2]
    ) / safe_square
    damping = 1.0 + VISCOSITY * TIME_STEP * square
    solved = jnp.stack(
        [
            (spectrum[:, component] - waves[component] * projected) / damping
            for component in range(3)
        ],
        axis=1,
    )
    solved = complex_pass(solved, 2, False)
    solved = lax.all_to_all(solved, "slab", split_axis=2, concat_axis=3, tiled=True)
    solved = complex_pass(solved, 3, False)
    solved = lax.all_to_all(solved, "grp", split_axis=3, concat_axis=4, tiled=True)
    flat_real = solved[0].reshape(-1, width_y)
    flat_imag = solved[1].reshape(-1, width_y)
    combined = jnp.dot(flat_real, cosine_y, precision=lax.Precision.HIGHEST) - jnp.dot(
        flat_imag, sine_y, precision=lax.Precision.HIGHEST
    )
    new_velocity = combined.reshape(velocity.shape) / (width_y * total_x * total_z)
    return (new_velocity, new_fields)


ROW_TILE = 16
END_ROWS = 8


def real_basis(length):
    half = length // 2
    cell = np.arange(length)
    wave = np.arange(half)
    angle = (cell[:, None] * wave[None, :] % length) * (2.0 * math.pi / length)
    sine = np.sin(angle)
    sine[:, 0] = np.where(cell % 2 == 0, 1.0, -1.0)
    return np.concatenate([np.cos(angle), sine], axis=1)


def split_tables(*tables):
    parts = []
    for table in tables:
        high = table.astype(jnp.bfloat16)
        parts += [high, (table - high.astype(np.float64)).astype(jnp.bfloat16)]
    return jnp.asarray(np.stack(parts))


def split_value(value):
    high = value.astype(jnp.bfloat16)
    return high, (value - high.astype(jnp.float32)).astype(jnp.bfloat16)


def dot_split(left, right, dims):
    def one(a, b):
        return lax.dot_general(a, b, (dims, ((), ())), preferred_element_type=jnp.float32)

    return one(left[0], right[0]) + (one(left[0], right[1]) + one(left[1], right[0]))


def row_index(shape):
    return lax.broadcasted_iota(jnp.int32, shape, 0)


def lane_index(shape):
    return lax.broadcasted_iota(jnp.int32, shape, 1)


def row_after(block, last):
    rows = block.shape[0]
    moved = pltpu.roll(block, rows - 1, 0)
    return jnp.where(row_index(block.shape) == rows - 1, last, moved)


def row_before(block, first):
    moved = pltpu.roll(block, 1, 0)
    return jnp.where(row_index(block.shape) == 0, first, moved)


def lane_difference(block):
    lanes = block.shape[1]
    return pltpu.roll(block, lanes - 1, 1) - pltpu.roll(block, 1, 1)


def run_kernel(body, outs, args, scalars=(), scratch=(), flops=0, far=()):
    leaves = list(args) + jax.tree.leaves(outs)
    leaves += [leaf for leaf in scratch if leaf.memory_space == pltpu.VMEM]
    held = sum(math.prod(leaf.shape) * jnp.dtype(leaf.dtype).itemsize for leaf in leaves)
    args = [
        pltpu.with_memory_space_constraint(arg, pltpu.HBM) if number in far else arg
        for number, arg in enumerate(args)
    ]
    in_specs = [pl.BlockSpec(memory_space=pltpu.SMEM) for _ in scalars]
    in_specs += [
        pl.BlockSpec(memory_space=pltpu.HBM if number in far else pltpu.VMEM)
        for number in range(len(args))
    ]
    return pl.pallas_call(
        body,
        out_shape=outs,
        in_specs=in_specs,
        out_specs=jax.tree.map(lambda _: pl.BlockSpec(memory_space=pltpu.VMEM), outs),
        scratch_shapes=scratch,
        compiler_params=pltpu.CompilerParams(vmem_limit_bytes=held + (4 << 20)),
        cost_estimate=pl.CostEstimate(flops=flops, bytes_accessed=held, transcendentals=0),
    )(*scalars, *args)


def rim_rows(members):
    return -(-(6 * members + 18) // ROW_TILE) * ROW_TILE


def pack_rows(fields, flow, grp_index, groups):
    members, dims, size_x, size_y = fields.shape
    rows = size_x // groups
    planes = members * dims
    rim = rim_rows(members)
    shape = jax.ShapeDtypeStruct((planes * rows + rim, size_y), fields.dtype)

    def pack(index, source, motion, *refs):
        targets, singles = refs[:groups], refs[groups : groups + dims]
        edges, ends, copied, fetched, ended, alone = refs[groups + dims :]
        last = motion.shape[1] - END_ROWS
        moves = [
            pltpu.make_async_copy(
                motion.at[:, first : first + END_ROWS, :], ends.at[side], ended.at[side]
            )
            for side, first in enumerate((0, last))
        ]
        for shift in range(groups):
            block = (index[0] + shift) % groups
            start = pl.multiple_of(block * rows, rows)
            above = pl.multiple_of((block + groups - 1) % groups * rows + rows - ROW_TILE, ROW_TILE)
            below = pl.multiple_of((block + 1) % groups * rows, rows)
            for side, place in enumerate((above, below)):
                moves.append(
                    pltpu.make_async_copy(
                        source.at[:, :, pl.ds(place, ROW_TILE), :],
                        edges.at[shift, side],
                        fetched.at[shift, side],
                    )
                )
            for plane in range(planes):
                moves.append(
                    pltpu.make_async_copy(
                        source.at[plane // dims, plane % dims, pl.ds(start, rows), :],
                        targets[shift].at[plane * rows : (plane + 1) * rows, :],
                        copied.at[shift, plane],
                    )
                )
        lone = [
            pltpu.make_async_copy(source.at[:, dim], singles[dim], alone.at[dim])
            for dim in range(dims)
        ]
        for move in moves + lone:
            move.start()
        place = row_index((rim, size_y))
        common = jnp.zeros((rim, size_y), jnp.float32)
        slot = 2 * planes
        for move in moves[:2]:
            move.wait()
        for side, line in enumerate((0, END_ROWS - 1)):
            for dim in range(dims):
                rest = ends[side, dim][line : line + 1, :]
                for _ in range(3):
                    part = rest.astype(jnp.bfloat16).astype(jnp.float32)
                    rest = rest - part
                    common = jnp.where(place == slot, part, common)
                    slot += 1
        for move in moves[2:]:
            move.wait()
        for shift in range(groups):
            edge = common
            for member in range(members):
                for dim in range(dims):
                    top = edges[shift, 0, member, dim].astype(jnp.float32)
                    bottom = edges[shift, 1, member, dim].astype(jnp.float32)
                    slot = dim * 2 * members + member * 2
                    edge = jnp.where(place == slot, top[ROW_TILE - 1 :], edge)
                    edge = jnp.where(place == slot + 1, bottom[:1], edge)
            targets[shift][planes * rows :, :] = edge.astype(fields.dtype)
        for move in lone:
            move.wait()

    return run_kernel(
        pack,
        [shape] * groups
        + [jax.ShapeDtypeStruct((members, size_x, size_y), fields.dtype)] * dims,
        [fields, flow],
        [grp_index],
        scratch=[
            pltpu.VMEM((groups, 2, members, dims, ROW_TILE, size_y), fields.dtype),
            pltpu.VMEM((2, 3, END_ROWS, size_y), flow.dtype),
            pltpu.SemaphoreType.DMA((groups, planes)),
            pltpu.SemaphoreType.DMA((groups, 2)),
            pltpu.SemaphoreType.DMA((2,)),
            pltpu.SemaphoreType.DMA((dims,)),
        ],
        far=(0, 1),
    )


def force_rows(blocks, motion, near, far, sign, table, members, field_total):
    rows, size_y = motion.shape[1:]
    planes = 3 * members
    rim = rim_rows(members)

    def stress_of(sums):
        stretch = stretch_factor((sums[0] + sums[1] + sums[2]) / field_total)
        return stretch, [
            POLY_MODULUS * (stretch * sums[slot] / field_total - (1.0 if first == second else 0.0))
            for slot, (first, second) in enumerate(TENSOR_PAIRS)
        ]

    def force(signs, *refs):
        parts = refs[: len(blocks)]
        flow, pair, other, tables, out, late, stress, stack = refs[len(blocks) :]
        side = signs[0].astype(jnp.float32)
        for start in range(0, rows, ROW_TILE):
            sums = [None] * 6
            for part in parts:
                for member in range(members):
                    vector = [
                        part[(member * 3 + dim) * rows + start :][:ROW_TILE, :].astype(jnp.float32)
                        if False
                        else part[
                            (member * 3 + dim) * rows + start : (member * 3 + dim) * rows
                            + start
                            + ROW_TILE,
                            :,
                        ].astype(jnp.float32)
                        for dim in range(3)
                    ]
                    for slot, (first, second) in enumerate(TENSOR_PAIRS):
                        term = vector[first] * vector[second]
                        sums[slot] = term if sums[slot] is None else sums[slot] + term
            stretch, values = stress_of(sums)
            late[3, start : start + ROW_TILE, :] = stretch
            for slot in range(6):
                stress[slot, start : start + ROW_TILE, :] = values[slot]
        sums = [None] * 6
        lines = []
        for part in parts:
            edge = part[planes * rows : planes * rows + rim, :].astype(jnp.float32)
            lines.append(edge[2 * planes :])
            vector = [edge[dim * 2 * members : (dim + 1) * 2 * members] for dim in range(3)]
            for slot, (first, second) in enumerate(TENSOR_PAIRS):
                term = vector[first] * vector[second]
                sums[slot] = term if sums[slot] is None else sums[slot] + term
        sums = [
            sum(value[2 * member : 2 * member + 2] for member in range(members)) for value in sums
        ]
        edges = stress_of(sums)[1]
        bottom = [sum(lines[-1][3 * c + t : 3 * c + t + 1] for t in range(3)) for c in range(3)]
        top = [sum(lines[1][9 + 3 * c + t : 10 + 3 * c + t] for t in range(3)) for c in range(3)]
        half = 0.5 * TIME_STEP
        place = {0: 0, 1: 1, 2: 4}
        for component in range(3):
            slot_x = pair_slot(component, 0)
            slot_y = pair_slot(component, 1)
            slot_z = pair_slot(component, 2)
            value = stress[slot_x]
            total = row_after(value, edges[slot_x][1:2]) - row_before(value, edges[slot_x][0:1])
            total = total + lane_difference(stress[slot_y])
            own = flow[component]
            total = total - flow[0] * (
                row_after(own, bottom[component]) - row_before(own, top[component])
            )
            total = total - flow[1] * lane_difference(own)
            rise = side * (pair[component] - other[component])
            late[component] = 0.5 * rise
            total = total - flow[2] * rise
            spot = place[component]
            stack[spot * rows : (spot + 1) * rows, :] = own + half * total
            spot = spot + (2 if component < 2 else 1)
            stack[spot * rows : (spot + 1) * rows, :] = half * stress[slot_z]
        out[...] = dot_split((tables[0], tables[1]), split_value(stack[...]), ((1,), (1,)))

    return run_kernel(
        force,
        [
            jax.ShapeDtypeStruct((size_y, 6 * rows), jnp.float32),
            jax.ShapeDtypeStruct((4, rows, size_y), jnp.float32),
        ],
        [*blocks, motion, near, far, table],
        [sign],
        scratch=[
            pltpu.VMEM((6, rows, size_y), jnp.float32),
            pltpu.VMEM((6 * rows, size_y), jnp.float32),
        ],
    )


def solve_pencil(pencil, device_index, table, groups, total_z, size_y):
    block = pencil.shape[1]
    pairs = block // 2
    rows = pencil.shape[2] // 6
    size_x = rows * groups
    half_x = size_x // 2
    half_z = total_z // 2
    basis_z = real_basis(total_z)
    lines = total_z * block
    step_x = 2.0 * math.pi / size_x
    step_y = 2.0 * math.pi / size_y
    step_z = 2.0 * math.pi / total_z

    def join(first, second, lane):
        return jnp.where(lane < rows, first, pltpu.roll(second, rows, 1))

    def solve(index, source, tables, out, stack, result):
        lane = lane_index((block, 2 * rows))
        for pair in range(groups // 2):
            both = []
            for side in range(2):
                group = 2 * pair + side
                tiles = [
                    [
                        source[group * total_z + z, :, t * 2 * rows : (t + 1) * 2 * rows]
                        for t in range(3)
                    ]
                    for z in range(total_z)
                ]
                both.append(
                    [
                        (
                            tiles[z][0] + tiles[(z + 1) % total_z][1] - tiles[z - 1][1],
                            tiles[z][2]
                            + pltpu.roll(tiles[(z + 1) % total_z][2] - tiles[z - 1][2], rows, 1),
                        )
                        for z in range(total_z)
                    ]
                )
            columns = slice(pair * 2 * rows, (pair + 1) * 2 * rows)
            for z in range(total_z):
                (first, third), (first_b, third_b) = both[0][z], both[1][z]
                line = z * block
                stack[line : line + block, columns] = join(first, first_b, lane)
                stack[lines + line : lines + line + block, columns] = jnp.where(
                    lane < rows, pltpu.roll(first, rows, 1), first_b
                )
                stack[2 * lines + line : 2 * lines + line + block, columns] = join(
                    third, third_b, lane
                )
        table_x = (tables[2], tables[3])
        result[...] = dot_split(split_value(stack[...]), table_x, ((1,), (0,)))

        shape = (block, size_x)
        lane = lane_index(shape)
        row = row_index(shape)
        wave = (lane % half_x).astype(jnp.float32) * step_x
        nyquist_x = jnp.where(lane == half_x, math.pi, 0.0)
        swap_x = jnp.where(lane < half_x, wave, -wave)
        square_x = wave * wave + nyquist_x * nyquist_x
        weight_x = jnp.where(lane % half_x == 0, 1.0, 2.0)
        number = index[0] * pairs + row % pairs
        wave = number.astype(jnp.float32) * step_y
        nyquist_y = jnp.where((number == 0) & (row >= pairs), math.pi, 0.0)
        swap_y = jnp.where(row < pairs, wave, -wave)
        square_y = wave * wave + nyquist_y * nyquist_y
        weight_y = jnp.where(number == 0, 1.0, 2.0)
        square_xy = square_x + square_y
        scale = weight_x * weight_y / (size_x * size_y * total_z)

        def along_x(value):
            return swap_x * pltpu.roll(value, half_x, 1)

        def along_y(value):
            return swap_y * pltpu.roll(value, pairs, 0)

        waves = []
        for component in range(3):
            planes = [
                result[component * lines + z * block : component * lines + (z + 1) * block, :]
                for z in range(total_z)
            ]
            waves.append(
                [
                    sum(float(basis_z[z, k]) * planes[z] for z in range(total_z))
                    for k in range(total_z)
                ]
            )

        def partner(k):
            if k % half_z == 0:
                return k, 0.0
            return (k + half_z, step_z * k) if k < half_z else (k - half_z, -step_z * (k - half_z))

        potential = []
        factors = []
        extra = []
        for k in range(total_z):
            wave_z = step_z * (k % half_z) if k != half_z else math.pi
            square = square_xy + wave_z * wave_z
            safe = jnp.where(square > 0, square, 1.0)
            other, factor = partner(k)
            total = along_x(waves[0][k]) + along_y(waves[1][k])
            if factor != 0.0:
                total = total + factor * waves[2][other]
            potential.append(total / safe)
            nyquist = nyquist_x * waves[0][k] + nyquist_y * waves[1][k]
            if k == half_z:
                nyquist = nyquist + math.pi * waves[2][k]
            extra.append(nyquist / safe)
            weight_z = 1.0 if k % half_z == 0 else 2.0
            factors.append(scale * weight_z / (1.0 + VISCOSITY * TIME_STEP * square))
        solved = [[], [], []]
        for k in range(total_z):
            other, factor = partner(k)
            solved[0].append(
                factors[k] * (waves[0][k] + along_x(potential[k]) - nyquist_x * extra[k])
            )
            solved[1].append(
                factors[k] * (waves[1][k] + along_y(potential[k]) - nyquist_y * extra[k])
            )
            value = waves[2][k]
            if factor != 0.0:
                value = value + factor * potential[other]
            if k == half_z:
                value = value - math.pi * extra[k]
            solved[2].append(factors[k] * value)
        for component in range(3):
            for z in range(total_z):
                line = component * lines + z * block
                stack[line : line + block, :] = sum(
                    float(basis_z[z, k]) * solved[component][k] for k in range(total_z)
                )
        result[...] = dot_split(split_value(stack[...]), table_x, ((1,), (1,)))
        lane = lane_index((block, 2 * rows))
        for group in range(groups):
            columns = slice(group // 2 * 2 * rows, (group // 2 + 1) * 2 * rows)
            for z in range(total_z):
                line = z * block
                first, second, third = [
                    result[c * lines + line : c * lines + line + block, columns] for c in range(3)
                ]
                if group % 2 == 0:
                    front = join(first, second, lane)
                else:
                    front = jnp.where(lane < rows, pltpu.roll(first, rows, 1), second)
                    third = pltpu.roll(third, rows, 1)
                out[group * total_z + z, :, : 2 * rows] = front
                out[group * total_z + z, :, 2 * rows :] = third

    return run_kernel(
        solve,
        jax.ShapeDtypeStruct((groups * total_z, block, 4 * rows), jnp.float32),
        [pencil, table],
        [device_index],
        scratch=[
            pltpu.VMEM((3 * lines, size_x), jnp.float32),
            pltpu.VMEM((3 * lines, size_x), jnp.float32),
        ],
    )


def rows_from_waves(spectra, table, rows):
    size_y = table.shape[2]

    def synthesise(source, tables, out):
        turned = source[...].T[: 3 * rows]
        value = dot_split(split_value(turned), (tables[0], tables[1]), ((1,), (0,)))
        for component in range(3):
            out[component, 0] = value[component * rows : (component + 1) * rows]

    return run_kernel(
        synthesise,
        jax.ShapeDtypeStruct((3, 1, rows, size_y), jnp.float32),
        [spectra, table],
    )


def advance_fields(fields, near, far, motions, lates, noise, grp_index, offsets, sign):
    members, _, size_x, size_y = fields.shape
    count = len(offsets)
    rows = size_x // count
    steps = size_x // ROW_TILE
    half = 0.5 * TIME_STEP

    def advance(spot, signs, kick, own, *refs):
        close, remote, refs = refs[:3], refs[3:6], refs[6:]
        flows, others, (out, plane) = refs[:count], refs[count : 2 * count], refs[2 * count :]
        for number in range(count):
            start = pl.multiple_of((spot[0] ^ offsets[number]) * rows, rows)
            for slot in range(3):
                plane[slot, pl.ds(start, rows), :] = flows[number][slot]
            for slot in range(4):
                plane[3 + slot, pl.ds(start, rows), :] = others[number][slot]
        side = signs[0].astype(jnp.float32)

        def step(number, carry):
            start = pl.multiple_of(number * ROW_TILE, ROW_TILE)
            before = pl.multiple_of((number + steps - 1) % steps * ROW_TILE, ROW_TILE)
            after = pl.multiple_of((number + 1) % steps * ROW_TILE, ROW_TILE)
            here = pl.ds(start, ROW_TILE)
            speed = [half * plane[c, here, :] for c in range(3)]
            slope = []
            for c in range(3):
                first = half * plane[c, pl.ds(before, ROW_TILE), :][ROW_TILE - 1 :]
                last = half * plane[c, pl.ds(after, ROW_TILE), :][:1]
                slope.append(
                    (
                        row_after(speed[c], last) - row_before(speed[c], first),
                        lane_difference(speed[c]),
                        TIME_STEP * plane[3 + c, here, :],
                    )
                )
            keep = 1.0 - (TIME_STEP / (2.0 * RELAX_TIME)) * plane[6, here, :]
            lift = side * speed[2]
            for member in range(members):
                vector = [own[member, c, here, :].astype(jnp.float32) for c in range(3)]
                for c in range(3):
                    first = own[member, c, pl.ds(before, ROW_TILE), :].astype(jnp.float32)
                    last = own[member, c, pl.ds(after, ROW_TILE), :].astype(jnp.float32)
                    value = vector[c]
                    rise = close[c][member, here, :].astype(jnp.float32)
                    rise = rise - remote[c][member, here, :].astype(jnp.float32)
                    total = keep * value + NOISE_SCALE * kick[member, c]
                    for j in range(3):
                        total = total + slope[c][j] * vector[j]
                    total = total - speed[0] * (
                        row_after(value, last[:1]) - row_before(value, first[ROW_TILE - 1 :])
                    )
                    total = total - speed[1] * lane_difference(value)
                    total = total - lift * rise
                    out[member, c, here, :] = total.astype(out.dtype)
            return carry

        lax.fori_loop(0, steps, step, 0)

    return run_kernel(
        advance,
        jax.ShapeDtypeStruct(fields.shape, fields.dtype),
        [fields, *near, *far, *motions, *lates],
        [grp_index, sign, noise],
        scratch=[pltpu.VMEM((7, size_x, size_y), jnp.float32)],
        flops=200 * members * size_x * size_y,
    )


def shifted(value, axis, step):
    count = lax.axis_size(axis)
    return lax.ppermute(value, axis, [(i, (i + step) % count) for i in range(count)])


def flipped(value, axis, bit):
    count = lax.axis_size(axis)
    return lax.ppermute(value, axis, [(i, i ^ bit) for i in range(count)])


def spread(value, axis):
    bit = lax.axis_size(axis) // 2
    found = [(0, value)]
    while bit:
        for offset, held in list(found):
            found.append((offset ^ bit, flipped(held, axis, bit)))
        bit //= 2
    return found


def pencil_shards(velocity, fields, noise):
    groups = lax.axis_size("grp")
    slabs = lax.axis_size("slab")
    grp_index = lax.axis_index("grp")
    slab_index = lax.axis_index("slab")
    members, _, _, size_x, size_y = fields.shape
    rows = velocity.shape[2]
    devices = groups * slabs
    block = size_y // devices
    half_block = block // 2
    order = np.concatenate(
        [
            np.concatenate([np.arange(half_block), size_y // 2 + np.arange(half_block)])
            + device * half_block
            for device in range(devices)
        ]
    )
    table = split_tables(np.ascontiguousarray(real_basis(size_y).T[order]), real_basis(size_x))

    flow = velocity[:, 0]
    plane = fields[:, :, 0]
    two_up = [(i, (i + (-2 if i % 2 else 2)) % slabs) for i in range(slabs)]
    sign = (1 - 2 * (slab_index & 1)).reshape(1)
    packed = pack_rows(plane, flow, grp_index.reshape(1), groups)
    blocks, parts = packed[:groups], packed[groups:]
    received = [blocks[0]]
    for d in range(1, groups):
        received.append(shifted(blocks[d], "grp", d))
    flow_near = flipped(flow, "slab", 1)
    flow_far = lax.ppermute(flow_near, "slab", two_up)
    two_down = [(target, source) for source, target in two_up]
    near = []
    for part in parts:
        near.append(flipped(part, "slab", 1))
    hopped = lax.ppermute(parts[0], "slab", two_down)
    far = [flipped(hopped, "slab", 1)]
    far.append(lax.ppermute(near[1], "slab", two_up))
    motions = spread(flow, "grp")
    spectra, late = force_rows(
        received, flow, flow_near, flow_far, sign, table, members, members * groups
    )
    lates = spread(late, "grp")
    pencil = lax.all_to_all(
        spectra.reshape(devices, block, 6 * rows),
        ("grp", "slab"),
        split_axis=0,
        concat_axis=0,
        tiled=True,
    )
    last, pencil = lax.optimization_barrier((near[2], pencil))
    far.append(lax.ppermute(last, "slab", two_up))
    device_index = (grp_index * slabs + slab_index).reshape(1)
    solved = solve_pencil(pencil, device_index, table, groups, slabs, size_y)
    new_fields = advance_fields(
        plane,
        near,
        far,
        [held for _, held in motions],
        [held for _, held in lates],
        noise,
        grp_index.reshape(1),
        [offset for offset, _ in motions],
        sign,
    )
    solved = lax.all_to_all(
        solved, ("grp", "slab"), split_axis=0, concat_axis=0, tiled=True
    )
    new_velocity = rows_from_waves(solved.reshape(size_y, 4 * rows), table, rows)
    return (new_velocity, new_fields[:, :, None])


def pencil_fits(mesh, velocity, fields):
    groups, slabs = mesh.shape["grp"], mesh.shape["slab"]
    size_z, size_x, size_y = velocity.shape[1:]
    return (
        size_z == slabs
        and slabs % 2 == 0
        and groups >= 2
        and groups & (groups - 1) == 0
        and size_y % (2 * groups * slabs) == 0
        and size_x % (groups * ROW_TILE) == 0
        and (2 * size_x // groups) % 128 == 0
        and fields.shape[0] % groups == 0
    )


def solution(mesh):
    specs = (P(None, "slab", "grp", None), P("grp", None, "slab", None, None), P("grp", None))

    def mapped(body):
        return jax.shard_map(body, mesh=mesh, in_specs=specs, out_specs=specs[:2], check_vma=False)

    def step(velocity, fields, noise):
        if not pencil_fits(mesh, velocity, fields):
            return mapped(shards)(velocity, fields, noise)
        return mapped(pencil_shards)(velocity, fields, noise)

    return step
```

```python
import math

import jax
import jax.numpy as jnp
import numpy as np
from jax import lax
from jax.experimental import pallas as pl
from jax.experimental.pallas import tpu as pltpu
from jax.sharding import PartitionSpec as P

TIME_STEP = 0.05
RELAX_TIME = 0.1
STRETCH_MAX = 36.0
POLY_MODULUS = 2.0
VISCOSITY = 0.2
NOISE_SCALE = math.sqrt(TIME_STEP / RELAX_TIME)
TENSOR_PAIRS = ((0, 0), (1, 1), (2, 2), (0, 1), (0, 2), (1, 2))


def extended(block, sides, width):
    for axis, dim in sides:
        count = lax.axis_size(axis)
        forward = [(i, i + 1) for i in range(count - 1)]
        forward.append((count - 1, 0))
        backward = [(target, source) for source, target in forward]
        low = lax.ppermute(
            lax.slice_in_dim(block, block.shape[dim] - width, None, axis=dim), axis, forward
        )
        high = lax.ppermute(lax.slice_in_dim(block, 0, width, axis=dim), axis, backward)
        block = jnp.concatenate([low, block, high], axis=dim)
    return block


def pair_slot(first_axis, second_axis):
    return TENSOR_PAIRS.index((min(first_axis, second_axis), max(first_axis, second_axis)))


def centred(values, axis):
    return (jnp.roll(values, -1, axis) - jnp.roll(values, 1, axis)) * 0.5


def stack_gradient(parts):
    return jnp.stack(
        [parts[direction][component] for component in range(3) for direction in range(3)]
    )


def pair_products(conform):
    return jnp.stack(
        [jnp.sum(conform[:, first] * conform[:, second], axis=0) for first, second in TENSOR_PAIRS]
    )


def stretch_factor(mean_square):
    return 1.0 / (1.0 - mean_square / STRETCH_MAX)


def poly_stress(sums, stretch, field_total):
    identity = jnp.array([1.0, 1.0, 1.0, 0.0, 0.0, 0.0], jnp.float32)[:, None, None, None]
    return POLY_MODULUS * (stretch * sums / field_total - identity)


def dft_tables(length):
    counter = jnp.arange(length, dtype=jnp.int32)
    phase = counter[:, None] * counter[None, :] % length
    angle = phase.astype(jnp.float32) * (2.0 * math.pi / length)
    return (jnp.cos(angle), jnp.sin(angle))


def along_axis(values, table, axis):
    letters = "abcdef"[: values.ndim]
    result = letters[:axis] + "k" + letters[axis + 1 :]
    return jnp.einsum(
        letters + "," + letters[axis] + "k->" + result,
        values,
        table,
        precision=lax.Precision.HIGHEST,
    )


def complex_pass(stacked, axis, forward):
    cosine, sine_table = dft_tables(stacked.shape[axis])
    cos_terms = along_axis(stacked, cosine, axis)
    sin_terms = along_axis(stacked, sine_table, axis)
    if forward:
        return jnp.stack([cos_terms[0] + sin_terms[1], cos_terms[1] - sin_terms[0]])
    return jnp.stack([cos_terms[0] - sin_terms[1], cos_terms[1] + sin_terms[0]])


def wavenumber(indices, length):
    signed = jnp.where(indices < length // 2, indices, indices - length)
    return signed.astype(jnp.float32) * (2.0 * math.pi / length)


def shards(velocity, fields, noise):
    grp_count = lax.axis_size("grp")
    grp_index = lax.axis_index("grp")
    slab_count = lax.axis_size("slab")
    slab_index = lax.axis_index("slab")
    field_total = fields.shape[0] * grp_count
    row_count = velocity.shape[2]
    row_start = grp_index * row_count
    width_y = velocity.shape[3]
    rimmed = extended(velocity, (("grp", 2), ("slab", 1)), 1)
    along_x = (rimmed[:, 1:-1, 2:, :] - rimmed[:, 1:-1, :-2, :]) * 0.5
    along_y = centred(velocity, 3)
    along_z = (rimmed[:, 2:, 1:-1, :] - rimmed[:, :-2, 1:-1, :]) * 0.5
    grad_rows = stack_gradient((along_x, along_y, along_z))
    grad_plane, vel_plane = (
        lax.all_gather(grad_rows, "grp", axis=2, tiled=True),
        lax.all_gather(velocity, "grp", axis=2, tiled=True),
    )
    field_rim = extended(fields, (("slab", 2),), 1)
    conform = fields.astype(jnp.float32)
    field_dz = (
        field_rim[:, :, 2:].astype(jnp.float32) - field_rim[:, :, :-2].astype(jnp.float32)
    ) * 0.5
    summed = lax.psum(pair_products(conform), "grp")
    stretch = stretch_factor((summed[0] + summed[1] + summed[2]) / field_total)
    stress_plane = poly_stress(summed, stretch, field_total)
    wrapped = jnp.concatenate(
        [stress_plane[:, :, -1:], stress_plane, stress_plane[:, :, :1]], axis=2
    )
    stress_rows = lax.dynamic_slice_in_dim(wrapped, row_start, row_count + 2, 2)
    stress_pad = extended(stress_rows, (("slab", 1),), 1)
    updated = []
    for component in range(3):
        member = conform[:, component]
        advect = (
            vel_plane[0] * centred(member, 2)
            + vel_plane[1] * centred(member, 3)
            + vel_plane[2] * field_dz[:, component]
        )
        stretching = sum(
            (
                grad_plane[3 * component + direction] * conform[:, direction]
                for direction in range(3)
            )
        )
        drift = stretching - advect - stretch * member / (2.0 * RELAX_TIME)
        updated.append(
            member + TIME_STEP * drift + NOISE_SCALE * noise[:, component][:, None, None, None]
        )
    new_fields = jnp.stack(updated, axis=1).astype(jnp.bfloat16)
    forcing = []
    for component in range(3):
        convect = sum(
            (velocity[direction] * grad_rows[3 * component + direction] for direction in range(3))
        )
        slot_x = pair_slot(component, 0)
        slot_y = pair_slot(component, 1)
        slot_z = pair_slot(component, 2)
        divergence = (stress_pad[slot_x, 1:-1, 2:, :] - stress_pad[slot_x, 1:-1, :-2, :]) * 0.5
        divergence = divergence + centred(stress_pad[slot_y, 1:-1, 1:-1, :], 2)
        divergence = (
            divergence + (stress_pad[slot_z, 2:, 1:-1, :] - stress_pad[slot_z, :-2, 1:-1, :]) * 0.5
        )
        forcing.append(velocity[component] + TIME_STEP * (divergence - convect))
    forcing = jnp.stack(forcing)
    cosine_y, sine_y = dft_tables(width_y)
    flat = forcing.reshape(-1, width_y)
    real_part = jnp.dot(flat, cosine_y, precision=lax.Precision.HIGHEST).reshape(forcing.shape)
    imag_part = -jnp.dot(flat, sine_y, precision=lax.Precision.HIGHEST).reshape(forcing.shape)
    spectrum = jnp.stack([real_part, imag_part])
    spectrum = lax.all_to_all(spectrum, "grp", split_axis=4, concat_axis=3, tiled=True)
    spectrum = complex_pass(spectrum, 3, True)
    spectrum = lax.all_to_all(spectrum, "slab", split_axis=3, concat_axis=2, tiled=True)
    spectrum = complex_pass(spectrum, 2, True)
    total_z = spectrum.shape[2]
    cols_x = spectrum.shape[3]
    cols_y = spectrum.shape[4]
    total_x = cols_x * slab_count
    total_y = cols_y * grp_count
    wave_z = wavenumber(jnp.arange(total_z, dtype=jnp.int32), total_z)[:, None, None]
    wave_x = wavenumber(slab_index * cols_x + jnp.arange(cols_x, dtype=jnp.int32), total_x)[
        None, :, None
    ]
    wave_y = wavenumber(grp_index * cols_y + jnp.arange(cols_y, dtype=jnp.int32), total_y)[
        None, None, :
    ]
    waves = (wave_x, wave_y, wave_z)
    square = wave_x * wave_x + wave_y * wave_y + wave_z * wave_z
    safe_square = jnp.where(square > 0, square, 1.0)
    projected = (
        wave_x * spectrum[:, 0] + wave_y * spectrum[:, 1] + wave_z * spectrum[:, 2]
    ) / safe_square
    damping = 1.0 + VISCOSITY * TIME_STEP * square
    solved = jnp.stack(
        [
            (spectrum[:, component] - waves[component] * projected) / damping
            for component in range(3)
        ],
        axis=1,
    )
    solved = complex_pass(solved, 2, False)
    solved = lax.all_to_all(solved, "slab", split_axis=2, concat_axis=3, tiled=True)
    solved = complex_pass(solved, 3, False)
    solved = lax.all_to_all(solved, "grp", split_axis=3, concat_axis=4, tiled=True)
    flat_real = solved[0].reshape(-1, width_y)
    flat_imag = solved[1].reshape(-1, width_y)
    combined = jnp.dot(flat_real, cosine_y, precision=lax.Precision.HIGHEST) - jnp.dot(
        flat_imag, sine_y, precision=lax.Precision.HIGHEST
    )
    new_velocity = combined.reshape(velocity.shape) / (width_y * total_x * total_z)
    return (new_velocity, new_fields)


ROW_TILE = 16
END_ROWS = 8


def real_basis(length):
    half = length // 2
    cell = np.arange(length)
    wave = np.arange(half)
    angle = (cell[:, None] * wave[None, :] % length) * (2.0 * math.pi / length)
    sine = np.sin(angle)
    sine[:, 0] = np.where(cell % 2 == 0, 1.0, -1.0)
    return np.concatenate([np.cos(angle), sine], axis=1)


def split_tables(*tables):
    parts = []
    for table in tables:
        high = table.astype(jnp.bfloat16)
        parts += [high, (table - high.astype(np.float64)).astype(jnp.bfloat16)]
    return jnp.asarray(np.stack(parts))


def split_value(value):
    high = value.astype(jnp.bfloat16)
    return high, (value - high.astype(jnp.float32)).astype(jnp.bfloat16)


def dot_split(left, right, dims):
    def one(a, b):
        return lax.dot_general(a, b, (dims, ((), ())), preferred_element_type=jnp.float32)

    return one(left[0], right[0]) + (one(left[0], right[1]) + one(left[1], right[0]))


def row_index(shape):
    return lax.broadcasted_iota(jnp.int32, shape, 0)


def lane_index(shape):
    return lax.broadcasted_iota(jnp.int32, shape, 1)


def row_after(block, last):
    rows = block.shape[0]
    moved = pltpu.roll(block, rows - 1, 0)
    return jnp.where(row_index(block.shape) == rows - 1, last, moved)


def row_before(block, first):
    moved = pltpu.roll(block, 1, 0)
    return jnp.where(row_index(block.shape) == 0, first, moved)


def lane_difference(block):
    lanes = block.shape[1]
    return pltpu.roll(block, lanes - 1, 1) - pltpu.roll(block, 1, 1)


def run_kernel(body, outs, args, scalars=(), scratch=(), flops=0, far=(), far_outs=(), aliases=None):
    leaves = list(args) + jax.tree.leaves(outs)
    leaves += [leaf for leaf in scratch if leaf.memory_space == pltpu.VMEM]
    held = sum(math.prod(leaf.shape) * jnp.dtype(leaf.dtype).itemsize for leaf in leaves)
    args = [
        pltpu.with_memory_space_constraint(arg, pltpu.HBM) if number in far else arg
        for number, arg in enumerate(args)
    ]
    spaces = jax.tree.map(lambda _: pl.BlockSpec(memory_space=pltpu.VMEM), outs)
    for number in far_outs:
        spaces[number] = pl.BlockSpec(memory_space=pltpu.HBM)
    in_specs = [pl.BlockSpec(memory_space=pltpu.SMEM) for _ in scalars]
    in_specs += [
        pl.BlockSpec(memory_space=pltpu.HBM if number in far else pltpu.VMEM)
        for number in range(len(args))
    ]
    return pl.pallas_call(
        body,
        out_shape=outs,
        in_specs=in_specs,
        out_specs=spaces,
        scratch_shapes=scratch,
        input_output_aliases=aliases or {},
        compiler_params=pltpu.CompilerParams(vmem_limit_bytes=held + (4 << 20)),
        cost_estimate=pl.CostEstimate(flops=flops, bytes_accessed=held, transcendentals=0),
    )(*scalars, *args)


def rim_rows(members):
    return -(-(6 * members + 18) // ROW_TILE) * ROW_TILE


def pack_rows(fields, flow, grp_index, groups):
    members, dims, size_x, size_y = fields.shape
    rows = size_x // groups
    planes = members * dims
    rim = rim_rows(members)
    shape = jax.ShapeDtypeStruct((planes * rows + rim, size_y), fields.dtype)

    def pack(index, source, motion, *refs):
        targets, singles = refs[:groups], refs[groups : groups + dims]
        edges, ends, copied, fetched, ended, alone = refs[groups + dims :]
        last = motion.shape[1] - END_ROWS
        moves = [
            pltpu.make_async_copy(
                motion.at[:, first : first + END_ROWS, :], ends.at[side], ended.at[side]
            )
            for side, first in enumerate((0, last))
        ]
        for shift in range(groups):
            block = (index[0] + shift) % groups
            start = pl.multiple_of(block * rows, rows)
            above = pl.multiple_of((block + groups - 1) % groups * rows + rows - ROW_TILE, ROW_TILE)
            below = pl.multiple_of((block + 1) % groups * rows, rows)
            for side, place in enumerate((above, below)):
                moves.append(
                    pltpu.make_async_copy(
                        source.at[:, :, pl.ds(place, ROW_TILE), :],
                        edges.at[shift, side],
                        fetched.at[shift, side],
                    )
                )
            for plane in range(planes):
                moves.append(
                    pltpu.make_async_copy(
                        source.at[plane // dims, plane % dims, pl.ds(start, rows), :],
                        targets[shift].at[plane * rows : (plane + 1) * rows, :],
                        copied.at[shift, plane],
                    )
                )
        lone = [
            pltpu.make_async_copy(source.at[:, dim], singles[dim], alone.at[dim])
            for dim in range(dims)
        ]
        for move in moves + lone:
            move.start()
        place = row_index((rim, size_y))
        common = jnp.zeros((rim, size_y), jnp.float32)
        slot = 2 * planes
        for move in moves[:2]:
            move.wait()
        for side, line in enumerate((0, END_ROWS - 1)):
            for dim in range(dims):
                rest = ends[side, dim][line : line + 1, :]
                for _ in range(3):
                    part = rest.astype(jnp.bfloat16).astype(jnp.float32)
                    rest = rest - part
                    common = jnp.where(place == slot, part, common)
                    slot += 1
        for move in moves[2:]:
            move.wait()
        for shift in range(groups):
            edge = common
            for member in range(members):
                for dim in range(dims):
                    top = edges[shift, 0, member, dim].astype(jnp.float32)
                    bottom = edges[shift, 1, member, dim].astype(jnp.float32)
                    slot = dim * 2 * members + member * 2
                    edge = jnp.where(place == slot, top[ROW_TILE - 1 :], edge)
                    edge = jnp.where(place == slot + 1, bottom[:1], edge)
            targets[shift][planes * rows :, :] = edge.astype(fields.dtype)
        for move in lone:
            move.wait()

    return run_kernel(
        pack,
        [shape] * groups
        + [jax.ShapeDtypeStruct((members, size_x, size_y), fields.dtype)] * dims,
        [fields, flow],
        [grp_index],
        scratch=[
            pltpu.VMEM((groups, 2, members, dims, ROW_TILE, size_y), fields.dtype),
            pltpu.VMEM((2, 3, END_ROWS, size_y), flow.dtype),
            pltpu.SemaphoreType.DMA((groups, planes)),
            pltpu.SemaphoreType.DMA((groups, 2)),
            pltpu.SemaphoreType.DMA((2,)),
            pltpu.SemaphoreType.DMA((dims,)),
        ],
        far=(0, 1),
    )


def force_rows(blocks, motion, near, far, sign, table, members, field_total):
    rows, size_y = motion.shape[1:]
    planes = 3 * members
    rim = rim_rows(members)

    def stress_of(sums):
        stretch = stretch_factor((sums[0] + sums[1] + sums[2]) / field_total)
        return stretch, [
            POLY_MODULUS * (stretch * sums[slot] / field_total - (1.0 if first == second else 0.0))
            for slot, (first, second) in enumerate(TENSOR_PAIRS)
        ]

    def force(signs, *refs):
        parts = refs[: len(blocks)]
        flow, pair, other, tables, out, late, stress, stack = refs[len(blocks) :]
        side = signs[0].astype(jnp.float32)
        for start in range(0, rows, ROW_TILE):
            sums = [None] * 6
            for part in parts:
                for member in range(members):
                    vector = [
                        part[(member * 3 + dim) * rows + start :][:ROW_TILE, :].astype(jnp.float32)
                        if False
                        else part[
                            (member * 3 + dim) * rows + start : (member * 3 + dim) * rows
                            + start
                            + ROW_TILE,
                            :,
                        ].astype(jnp.float32)
                        for dim in range(3)
                    ]
                    for slot, (first, second) in enumerate(TENSOR_PAIRS):
                        term = vector[first] * vector[second]
                        sums[slot] = term if sums[slot] is None else sums[slot] + term
            stretch, values = stress_of(sums)
            late[3, start : start + ROW_TILE, :] = stretch
            for slot in range(6):
                stress[slot, start : start + ROW_TILE, :] = values[slot]
        sums = [None] * 6
        lines = []
        for part in parts:
            edge = part[planes * rows : planes * rows + rim, :].astype(jnp.float32)
            lines.append(edge[2 * planes :])
            vector = [edge[dim * 2 * members : (dim + 1) * 2 * members] for dim in range(3)]
            for slot, (first, second) in enumerate(TENSOR_PAIRS):
                term = vector[first] * vector[second]
                sums[slot] = term if sums[slot] is None else sums[slot] + term
        sums = [
            sum(value[2 * member : 2 * member + 2] for member in range(members)) for value in sums
        ]
        edges = stress_of(sums)[1]
        bottom = [sum(lines[-1][3 * c + t : 3 * c + t + 1] for t in range(3)) for c in range(3)]
        top = [sum(lines[1][9 + 3 * c + t : 10 + 3 * c + t] for t in range(3)) for c in range(3)]
        half = 0.5 * TIME_STEP
        place = {0: 0, 1: 1, 2: 4}
        for component in range(3):
            slot_x = pair_slot(component, 0)
            slot_y = pair_slot(component, 1)
            slot_z = pair_slot(component, 2)
            value = stress[slot_x]
            total = row_after(value, edges[slot_x][1:2]) - row_before(value, edges[slot_x][0:1])
            total = total + lane_difference(stress[slot_y])
            own = flow[component]
            total = total - flow[0] * (
                row_after(own, bottom[component]) - row_before(own, top[component])
            )
            total = total - flow[1] * lane_difference(own)
            rise = side * (pair[component] - other[component])
            late[component] = 0.5 * rise
            total = total - flow[2] * rise
            spot = place[component]
            stack[spot * rows : (spot + 1) * rows, :] = own + half * total
            spot = spot + (2 if component < 2 else 1)
            stack[spot * rows : (spot + 1) * rows, :] = half * stress[slot_z]
        out[...] = dot_split((tables[0], tables[1]), split_value(stack[...]), ((1,), (1,)))

    return run_kernel(
        force,
        [
            jax.ShapeDtypeStruct((size_y, 6 * rows), jnp.float32),
            jax.ShapeDtypeStruct((4, rows, size_y), jnp.float32),
        ],
        [*blocks, motion, near, far, table],
        [sign],
        scratch=[
            pltpu.VMEM((6, rows, size_y), jnp.float32),
            pltpu.VMEM((6 * rows, size_y), jnp.float32),
        ],
    )


def solve_pencil(pencil, device_index, table, groups, total_z, size_y):
    block = pencil.shape[1]
    pairs = block // 2
    rows = pencil.shape[2] // 6
    size_x = rows * groups
    half_x = size_x // 2
    half_z = total_z // 2
    basis_z = real_basis(total_z)
    lines = total_z * block
    step_x = 2.0 * math.pi / size_x
    step_y = 2.0 * math.pi / size_y
    step_z = 2.0 * math.pi / total_z

    def join(first, second, lane):
        return jnp.where(lane < rows, first, pltpu.roll(second, rows, 1))

    def solve(index, source, tables, out, stack, result):
        lane = lane_index((block, 2 * rows))
        for pair in range(groups // 2):
            both = []
            for side in range(2):
                group = 2 * pair + side
                tiles = [
                    [
                        source[group * total_z + z, :, t * 2 * rows : (t + 1) * 2 * rows]
                        for t in range(3)
                    ]
                    for z in range(total_z)
                ]
                both.append(
                    [
                        (
                            tiles[z][0] + tiles[(z + 1) % total_z][1] - tiles[z - 1][1],
                            tiles[z][2]
                            + pltpu.roll(tiles[(z + 1) % total_z][2] - tiles[z - 1][2], rows, 1),
                        )
                        for z in range(total_z)
                    ]
                )
            columns = slice(pair * 2 * rows, (pair + 1) * 2 * rows)
            for z in range(total_z):
                (first, third), (first_b, third_b) = both[0][z], both[1][z]
                line = z * block
                stack[line : line + block, columns] = join(first, first_b, lane)
                stack[lines + line : lines + line + block, columns] = jnp.where(
                    lane < rows, pltpu.roll(first, rows, 1), first_b
                )
                stack[2 * lines + line : 2 * lines + line + block, columns] = join(
                    third, third_b, lane
                )
        table_x = (tables[2], tables[3])
        result[...] = dot_split(split_value(stack[...]), table_x, ((1,), (0,)))

        shape = (block, size_x)
        lane = lane_index(shape)
        row = row_index(shape)
        wave = (lane % half_x).astype(jnp.float32) * step_x
        nyquist_x = jnp.where(lane == half_x, math.pi, 0.0)
        swap_x = jnp.where(lane < half_x, wave, -wave)
        square_x = wave * wave + nyquist_x * nyquist_x
        weight_x = jnp.where(lane % half_x == 0, 1.0, 2.0)
        number = index[0] * pairs + row % pairs
        wave = number.astype(jnp.float32) * step_y
        nyquist_y = jnp.where((number == 0) & (row >= pairs), math.pi, 0.0)
        swap_y = jnp.where(row < pairs, wave, -wave)
        square_y = wave * wave + nyquist_y * nyquist_y
        weight_y = jnp.where(number == 0, 1.0, 2.0)
        square_xy = square_x + square_y
        scale = weight_x * weight_y / (size_x * size_y * total_z)

        def along_x(value):
            return swap_x * pltpu.roll(value, half_x, 1)

        def along_y(value):
            return swap_y * pltpu.roll(value, pairs, 0)

        waves = []
        for component in range(3):
            planes = [
                result[component * lines + z * block : component * lines + (z + 1) * block, :]
                for z in range(total_z)
            ]
            waves.append(
                [
                    sum(float(basis_z[z, k]) * planes[z] for z in range(total_z))
                    for k in range(total_z)
                ]
            )

        def partner(k):
            if k % half_z == 0:
                return k, 0.0
            return (k + half_z, step_z * k) if k < half_z else (k - half_z, -step_z * (k - half_z))

        potential = []
        factors = []
        extra = []
        for k in range(total_z):
            wave_z = step_z * (k % half_z) if k != half_z else math.pi
            square = square_xy + wave_z * wave_z
            safe = jnp.where(square > 0, square, 1.0)
            other, factor = partner(k)
            total = along_x(waves[0][k]) + along_y(waves[1][k])
            if factor != 0.0:
                total = total + factor * waves[2][other]
            potential.append(total / safe)
            nyquist = nyquist_x * waves[0][k] + nyquist_y * waves[1][k]
            if k == half_z:
                nyquist = nyquist + math.pi * waves[2][k]
            extra.append(nyquist / safe)
            weight_z = 1.0 if k % half_z == 0 else 2.0
            factors.append(scale * weight_z / (1.0 + VISCOSITY * TIME_STEP * square))
        solved = [[], [], []]
        for k in range(total_z):
            other, factor = partner(k)
            solved[0].append(
                factors[k] * (waves[0][k] + along_x(potential[k]) - nyquist_x * extra[k])
            )
            solved[1].append(
                factors[k] * (waves[1][k] + along_y(potential[k]) - nyquist_y * extra[k])
            )
            value = waves[2][k]
            if factor != 0.0:
                value = value + factor * potential[other]
            if k == half_z:
                value = value - math.pi * extra[k]
            solved[2].append(factors[k] * value)
        for component in range(3):
            for z in range(total_z):
                line = component * lines + z * block
                stack[line : line + block, :] = sum(
                    float(basis_z[z, k]) * solved[component][k] for k in range(total_z)
                )
        result[...] = dot_split(split_value(stack[...]), table_x, ((1,), (1,)))
        lane = lane_index((block, 2 * rows))
        for group in range(groups):
            columns = slice(group // 2 * 2 * rows, (group // 2 + 1) * 2 * rows)
            for z in range(total_z):
                line = z * block
                held = [
                    result[c * lines + line : c * lines + line + block, columns] for c in range(3)
                ]
                turned = [pltpu.roll(value, rows, 1) for value in held]
                low, high = (held, turned) if group % 2 == 0 else (turned, held)
                tiles = (
                    jnp.where(lane < rows, low[0], high[1]),
                    jnp.where(lane < rows, low[2], pltpu.roll(high[0], pairs, 0)),
                    pltpu.roll(jnp.where(lane < rows, low[1], high[2]), pairs, 0),
                )
                for number, tile in enumerate(tiles):
                    spot = slice(number * 2 * rows, (number + 1) * 2 * rows)
                    out[group * total_z + z, :, spot] = tile[:pairs]

    return run_kernel(
        solve,
        jax.ShapeDtypeStruct((groups * total_z, pairs, 6 * rows), jnp.float32),
        [pencil, table],
        [device_index],
        scratch=[
            pltpu.VMEM((3 * lines, size_x), jnp.float32),
            pltpu.VMEM((3 * lines, size_x), jnp.float32),
        ],
    )


def rows_from_waves(spectra, table, rows):
    devices, pairs, lanes = spectra.shape
    size_y = table.shape[2]
    joined = max(8 // pairs, 1)

    def synthesise(source, tables, out, stack):
        for first in range(0, devices, joined):
            blocks = [source[device] for device in range(first, first + joined)]
            stack[first * pairs : (first + joined) * pairs, :] = jnp.concatenate(blocks, axis=0)
        turned = stack[...].T
        waves = jnp.concatenate([turned[: 3 * rows], turned[3 * rows :]], axis=1)
        value = dot_split(split_value(waves), (tables[2], tables[3]), ((1,), (1,)))
        for component in range(3):
            out[component, 0] = value[component * rows : (component + 1) * rows]

    return run_kernel(
        synthesise,
        jax.ShapeDtypeStruct((3, 1, rows, size_y), jnp.float32),
        [spectra, table],
        scratch=[pltpu.VMEM((devices * pairs, lanes), jnp.float32)],
    )


def advance_fields(fields, near, far, motions, lates, noise, grp_index, offsets, sign):
    members, _, size_x, size_y = fields.shape
    count = len(offsets)
    rows = size_x // count
    steps = size_x // ROW_TILE
    half = 0.5 * TIME_STEP

    def advance(spot, signs, kick, own, *refs):
        close, remote, refs = refs[:2], refs[2:4], refs[4:]
        flows, others, refs = refs[:count], refs[count : 2 * count], refs[2 * count :]
        out, rest, pace, plane, ready, sent = refs
        for number in range(count):
            start = pl.multiple_of((spot[0] ^ offsets[number]) * rows, rows)
            for slot in range(3):
                plane[slot, pl.ds(start, rows), :] = flows[number][slot]
            for slot in range(4):
                plane[3 + slot, pl.ds(start, rows), :] = others[number][slot]
        side = signs[0].astype(jnp.float32)

        def step(number, carry):
            start = pl.multiple_of(number * ROW_TILE, ROW_TILE)
            before = pl.multiple_of((number + steps - 1) % steps * ROW_TILE, ROW_TILE)
            after = pl.multiple_of((number + 1) % steps * ROW_TILE, ROW_TILE)
            here = pl.ds(start, ROW_TILE)
            speed = [half * plane[c, here, :] for c in range(3)]
            slope = []
            for c in range(3):
                first = half * plane[c, pl.ds(before, ROW_TILE), :][ROW_TILE - 1 :]
                last = half * plane[c, pl.ds(after, ROW_TILE), :][:1]
                slope.append(
                    (
                        row_after(speed[c], last) - row_before(speed[c], first),
                        lane_difference(speed[c]),
                        TIME_STEP * plane[3 + c, here, :],
                    )
                )
            keep = 1.0 - (TIME_STEP / (2.0 * RELAX_TIME)) * plane[6, here, :]
            lift = side * speed[2]
            pace[here, :] = lift
            for member in range(members):
                vector = [own[member, c, here, :].astype(jnp.float32) for c in range(3)]
                for c in range(3):
                    first = own[member, c, pl.ds(before, ROW_TILE), :].astype(jnp.float32)
                    last = own[member, c, pl.ds(after, ROW_TILE), :].astype(jnp.float32)
                    value = vector[c]
                    total = keep * value + NOISE_SCALE * kick[member, c]
                    for j in range(3):
                        total = total + slope[c][j] * vector[j]
                    total = total - speed[0] * (
                        row_after(value, last[:1]) - row_before(value, first[ROW_TILE - 1 :])
                    )
                    total = total - speed[1] * lane_difference(value)
                    if c == 2:
                        rest[member, here, :] = total
                        continue
                    rise = close[c][member, here, :].astype(jnp.float32)
                    rise = rise - remote[c][member, here, :].astype(jnp.float32)
                    ready[c, member, here, :] = (total - lift * rise).astype(ready.dtype)
            return carry

        lax.fori_loop(0, steps, step, 0)
        moves = [
            pltpu.make_async_copy(ready.at[c], out.at[:, c], sent.at[c]) for c in range(2)
        ]
        for move in moves:
            move.start()
        for move in moves:
            move.wait()

    return run_kernel(
        advance,
        [
            jax.ShapeDtypeStruct(fields.shape, fields.dtype),
            jax.ShapeDtypeStruct((members, size_x, size_y), jnp.float32),
            jax.ShapeDtypeStruct((size_x, size_y), jnp.float32),
        ],
        [fields, *near, *far, *motions, *lates],
        [grp_index, sign, noise],
        scratch=[
            pltpu.VMEM((7, size_x, size_y), jnp.float32),
            pltpu.VMEM((2, members, size_x, size_y), fields.dtype),
            pltpu.SemaphoreType.DMA((2,)),
        ],
        far_outs=(0,),
        flops=200 * members * size_x * size_y,
    )


def finish_fields(fields, rest, pace, near, far):
    members, size_x, size_y = rest.shape

    def finish(partial, speed, close, remote, _, out, ready, sent):
        for member in range(members):
            rise = close[member].astype(jnp.float32) - remote[member].astype(jnp.float32)
            ready[member] = (partial[member] - speed[...] * rise).astype(ready.dtype)
        move = pltpu.make_async_copy(ready, out.at[:, 2], sent)
        move.start()
        move.wait()

    return run_kernel(
        finish,
        [jax.ShapeDtypeStruct(fields.shape, fields.dtype)],
        [rest, pace, near, far, fields],
        scratch=[
            pltpu.VMEM((members, size_x, size_y), fields.dtype),
            pltpu.SemaphoreType.DMA(()),
        ],
        flops=4 * members * size_x * size_y,
        far=(4,),
        far_outs=(0,),
        aliases={4: 0},
    )[0]


def shifted(value, axis, step):
    count = lax.axis_size(axis)
    return lax.ppermute(value, axis, [(i, (i + step) % count) for i in range(count)])


def flipped(value, axis, bit):
    count = lax.axis_size(axis)
    return lax.ppermute(value, axis, [(i, i ^ bit) for i in range(count)])


def spread(value, axis):
    bit = lax.axis_size(axis) // 2
    found = [(0, value)]
    while bit:
        for offset, held in list(found):
            found.append((offset ^ bit, flipped(held, axis, bit)))
        bit //= 2
    return found


def pencil_shards(velocity, fields, noise):
    groups = lax.axis_size("grp")
    slabs = lax.axis_size("slab")
    grp_index = lax.axis_index("grp")
    slab_index = lax.axis_index("slab")
    members, _, _, size_x, size_y = fields.shape
    rows = velocity.shape[2]
    devices = groups * slabs
    block = size_y // devices
    half_block = block // 2
    order = np.concatenate(
        [
            np.concatenate([np.arange(half_block), size_y // 2 + np.arange(half_block)])
            + device * half_block
            for device in range(devices)
        ]
    )
    table = split_tables(np.ascontiguousarray(real_basis(size_y).T[order]), real_basis(size_x))

    flow = velocity[:, 0]
    plane = fields[:, :, 0]
    two_up = [(i, (i + (-2 if i % 2 else 2)) % slabs) for i in range(slabs)]
    sign = (1 - 2 * (slab_index & 1)).reshape(1)
    packed = pack_rows(plane, flow, grp_index.reshape(1), groups)
    blocks, parts = packed[:groups], packed[groups:]
    received = [blocks[0]]
    for d in range(1, groups):
        received.append(shifted(blocks[d], "grp", d))
    flow_near = flipped(flow, "slab", 1)
    flow_far = lax.ppermute(flow_near, "slab", two_up)
    two_down = [(target, source) for source, target in two_up]
    near = []
    for part in parts:
        near.append(flipped(part, "slab", 1))
    hopped = lax.ppermute(parts[0], "slab", two_down)
    far = [flipped(hopped, "slab", 1)]
    far.append(lax.ppermute(near[1], "slab", two_up))
    motions = spread(flow, "grp")
    spectra, late = force_rows(
        received, flow, flow_near, flow_far, sign, table, members, members * groups
    )
    lates = spread(late, "grp")
    pencil = lax.all_to_all(
        spectra.reshape(devices, block, 6 * rows),
        ("grp", "slab"),
        split_axis=0,
        concat_axis=0,
        tiled=True,
    )
    last, pencil = lax.optimization_barrier((near[2], pencil))
    far.append(lax.ppermute(last, "slab", two_up))
    device_index = (grp_index * slabs + slab_index).reshape(1)
    solved = solve_pencil(pencil, device_index, table, groups, slabs, size_y)
    new_fields, rest, pace = advance_fields(
        plane,
        near[:2],
        far[:2],
        [held for _, held in motions],
        [held for _, held in lates],
        noise,
        grp_index.reshape(1),
        [offset for offset, _ in motions],
        sign,
    )
    new_fields = finish_fields(new_fields, rest, pace, near[2], far[2])
    solved = lax.all_to_all(
        solved, ("grp", "slab"), split_axis=0, concat_axis=0, tiled=True
    )
    new_velocity = rows_from_waves(solved, table, rows)
    return (new_velocity, new_fields[:, :, None])


def pencil_fits(mesh, velocity, fields):
    groups, slabs = mesh.shape["grp"], mesh.shape["slab"]
    size_z, size_x, size_y = velocity.shape[1:]
    return (
        size_z == slabs
        and size_x == size_y
        and slabs % 2 == 0
        and groups >= 2
        and groups & (groups - 1) == 0
        and size_y % (2 * groups * slabs) == 0
        and size_x % (groups * ROW_TILE) == 0
        and (2 * size_x // groups) % 128 == 0
        and fields.shape[0] % groups == 0
    )


def solution(mesh):
    specs = (P(None, "slab", "grp", None), P("grp", None, "slab", None, None), P("grp", None))

    def mapped(body):
        return jax.shard_map(body, mesh=mesh, in_specs=specs, out_specs=specs[:2], check_vma=False)

    def step(velocity, fields, noise):
        if not pencil_fits(mesh, velocity, fields):
            return mapped(shards)(velocity, fields, noise)
        return mapped(pencil_shards)(velocity, fields, noise)

    return step
```

```python
import math

import jax
import jax.numpy as jnp
import numpy as np
from jax import lax
from jax.experimental import pallas as pl
from jax.experimental.pallas import tpu as pltpu
from jax.sharding import PartitionSpec as P

TIME_STEP = 0.05
RELAX_TIME = 0.1
STRETCH_MAX = 36.0
POLY_MODULUS = 2.0
VISCOSITY = 0.2
NOISE_SCALE = math.sqrt(TIME_STEP / RELAX_TIME)
TENSOR_PAIRS = ((0, 0), (1, 1), (2, 2), (0, 1), (0, 2), (1, 2))


def extended(block, sides, width):
    for axis, dim in sides:
        count = lax.axis_size(axis)
        forward = [(i, i + 1) for i in range(count - 1)]
        forward.append((count - 1, 0))
        backward = [(target, source) for source, target in forward]
        low = lax.ppermute(
            lax.slice_in_dim(block, block.shape[dim] - width, None, axis=dim), axis, forward
        )
        high = lax.ppermute(lax.slice_in_dim(block, 0, width, axis=dim), axis, backward)
        block = jnp.concatenate([low, block, high], axis=dim)
    return block


def pair_slot(first_axis, second_axis):
    return TENSOR_PAIRS.index((min(first_axis, second_axis), max(first_axis, second_axis)))


def centred(values, axis):
    return (jnp.roll(values, -1, axis) - jnp.roll(values, 1, axis)) * 0.5


def stack_gradient(parts):
    return jnp.stack(
        [parts[direction][component] for component in range(3) for direction in range(3)]
    )


def pair_products(conform):
    return jnp.stack(
        [jnp.sum(conform[:, first] * conform[:, second], axis=0) for first, second in TENSOR_PAIRS]
    )


def stretch_factor(mean_square):
    return 1.0 / (1.0 - mean_square / STRETCH_MAX)


def poly_stress(sums, stretch, field_total):
    identity = jnp.array([1.0, 1.0, 1.0, 0.0, 0.0, 0.0], jnp.float32)[:, None, None, None]
    return POLY_MODULUS * (stretch * sums / field_total - identity)


def dft_tables(length):
    counter = jnp.arange(length, dtype=jnp.int32)
    phase = counter[:, None] * counter[None, :] % length
    angle = phase.astype(jnp.float32) * (2.0 * math.pi / length)
    return (jnp.cos(angle), jnp.sin(angle))


def along_axis(values, table, axis):
    letters = "abcdef"[: values.ndim]
    result = letters[:axis] + "k" + letters[axis + 1 :]
    return jnp.einsum(
        letters + "," + letters[axis] + "k->" + result,
        values,
        table,
        precision=lax.Precision.HIGHEST,
    )


def complex_pass(stacked, axis, forward):
    cosine, sine_table = dft_tables(stacked.shape[axis])
    cos_terms = along_axis(stacked, cosine, axis)
    sin_terms = along_axis(stacked, sine_table, axis)
    if forward:
        return jnp.stack([cos_terms[0] + sin_terms[1], cos_terms[1] - sin_terms[0]])
    return jnp.stack([cos_terms[0] - sin_terms[1], cos_terms[1] + sin_terms[0]])


def wavenumber(indices, length):
    signed = jnp.where(indices < length // 2, indices, indices - length)
    return signed.astype(jnp.float32) * (2.0 * math.pi / length)


def shards(velocity, fields, noise):
    grp_count = lax.axis_size("grp")
    grp_index = lax.axis_index("grp")
    slab_count = lax.axis_size("slab")
    slab_index = lax.axis_index("slab")
    field_total = fields.shape[0] * grp_count
    row_count = velocity.shape[2]
    row_start = grp_index * row_count
    width_y = velocity.shape[3]
    rimmed = extended(velocity, (("grp", 2), ("slab", 1)), 1)
    along_x = (rimmed[:, 1:-1, 2:, :] - rimmed[:, 1:-1, :-2, :]) * 0.5
    along_y = centred(velocity, 3)
    along_z = (rimmed[:, 2:, 1:-1, :] - rimmed[:, :-2, 1:-1, :]) * 0.5
    grad_rows = stack_gradient((along_x, along_y, along_z))
    grad_plane, vel_plane = (
        lax.all_gather(grad_rows, "grp", axis=2, tiled=True),
        lax.all_gather(velocity, "grp", axis=2, tiled=True),
    )
    field_rim = extended(fields, (("slab", 2),), 1)
    conform = fields.astype(jnp.float32)
    field_dz = (
        field_rim[:, :, 2:].astype(jnp.float32) - field_rim[:, :, :-2].astype(jnp.float32)
    ) * 0.5
    summed = lax.psum(pair_products(conform), "grp")
    stretch = stretch_factor((summed[0] + summed[1] + summed[2]) / field_total)
    stress_plane = poly_stress(summed, stretch, field_total)
    wrapped = jnp.concatenate(
        [stress_plane[:, :, -1:], stress_plane, stress_plane[:, :, :1]], axis=2
    )
    stress_rows = lax.dynamic_slice_in_dim(wrapped, row_start, row_count + 2, 2)
    stress_pad = extended(stress_rows, (("slab", 1),), 1)
    updated = []
    for component in range(3):
        member = conform[:, component]
        advect = (
            vel_plane[0] * centred(member, 2)
            + vel_plane[1] * centred(member, 3)
            + vel_plane[2] * field_dz[:, component]
        )
        stretching = sum(
            (
                grad_plane[3 * component + direction] * conform[:, direction]
                for direction in range(3)
            )
        )
        drift = stretching - advect - stretch * member / (2.0 * RELAX_TIME)
        updated.append(
            member + TIME_STEP * drift + NOISE_SCALE * noise[:, component][:, None, None, None]
        )
    new_fields = jnp.stack(updated, axis=1).astype(jnp.bfloat16)
    forcing = []
    for component in range(3):
        convect = sum(
            (velocity[direction] * grad_rows[3 * component + direction] for direction in range(3))
        )
        slot_x = pair_slot(component, 0)
        slot_y = pair_slot(component, 1)
        slot_z = pair_slot(component, 2)
        divergence = (stress_pad[slot_x, 1:-1, 2:, :] - stress_pad[slot_x, 1:-1, :-2, :]) * 0.5
        divergence = divergence + centred(stress_pad[slot_y, 1:-1, 1:-1, :], 2)
        divergence = (
            divergence + (stress_pad[slot_z, 2:, 1:-1, :] - stress_pad[slot_z, :-2, 1:-1, :]) * 0.5
        )
        forcing.append(velocity[component] + TIME_STEP * (divergence - convect))
    forcing = jnp.stack(forcing)
    cosine_y, sine_y = dft_tables(width_y)
    flat = forcing.reshape(-1, width_y)
    real_part = jnp.dot(flat, cosine_y, precision=lax.Precision.HIGHEST).reshape(forcing.shape)
    imag_part = -jnp.dot(flat, sine_y, precision=lax.Precision.HIGHEST).reshape(forcing.shape)
    spectrum = jnp.stack([real_part, imag_part])
    spectrum = lax.all_to_all(spectrum, "grp", split_axis=4, concat_axis=3, tiled=True)
    spectrum = complex_pass(spectrum, 3, True)
    spectrum = lax.all_to_all(spectrum, "slab", split_axis=3, concat_axis=2, tiled=True)
    spectrum = complex_pass(spectrum, 2, True)
    total_z = spectrum.shape[2]
    cols_x = spectrum.shape[3]
    cols_y = spectrum.shape[4]
    total_x = cols_x * slab_count
    total_y = cols_y * grp_count
    wave_z = wavenumber(jnp.arange(total_z, dtype=jnp.int32), total_z)[:, None, None]
    wave_x = wavenumber(slab_index * cols_x + jnp.arange(cols_x, dtype=jnp.int32), total_x)[
        None, :, None
    ]
    wave_y = wavenumber(grp_index * cols_y + jnp.arange(cols_y, dtype=jnp.int32), total_y)[
        None, None, :
    ]
    waves = (wave_x, wave_y, wave_z)
    square = wave_x * wave_x + wave_y * wave_y + wave_z * wave_z
    safe_square = jnp.where(square > 0, square, 1.0)
    projected = (
        wave_x * spectrum[:, 0] + wave_y * spectrum[:, 1] + wave_z * spectrum[:, 2]
    ) / safe_square
    damping = 1.0 + VISCOSITY * TIME_STEP * square
    solved = jnp.stack(
        [
            (spectrum[:, component] - waves[component] * projected) / damping
            for component in range(3)
        ],
        axis=1,
    )
    solved = complex_pass(solved, 2, False)
    solved = lax.all_to_all(solved, "slab", split_axis=2, concat_axis=3, tiled=True)
    solved = complex_pass(solved, 3, False)
    solved = lax.all_to_all(solved, "grp", split_axis=3, concat_axis=4, tiled=True)
    flat_real = solved[0].reshape(-1, width_y)
    flat_imag = solved[1].reshape(-1, width_y)
    combined = jnp.dot(flat_real, cosine_y, precision=lax.Precision.HIGHEST) - jnp.dot(
        flat_imag, sine_y, precision=lax.Precision.HIGHEST
    )
    new_velocity = combined.reshape(velocity.shape) / (width_y * total_x * total_z)
    return (new_velocity, new_fields)


ROW_TILE = 16
END_ROWS = 8


def real_basis(length):
    half = length // 2
    cell = np.arange(length)
    wave = np.arange(half)
    angle = (cell[:, None] * wave[None, :] % length) * (2.0 * math.pi / length)
    sine = np.sin(angle)
    sine[:, 0] = np.where(cell % 2 == 0, 1.0, -1.0)
    return np.concatenate([np.cos(angle), sine], axis=1)


def split_tables(*tables):
    parts = []
    for table in tables:
        high = table.astype(jnp.bfloat16)
        parts += [high, (table - high.astype(np.float64)).astype(jnp.bfloat16)]
    return jnp.asarray(np.stack(parts))


def split_value(value):
    high = value.astype(jnp.bfloat16)
    return high, (value - high.astype(jnp.float32)).astype(jnp.bfloat16)


def dot_split(left, right, dims):
    def one(a, b):
        return lax.dot_general(a, b, (dims, ((), ())), preferred_element_type=jnp.float32)

    return one(left[0], right[0]) + (one(left[0], right[1]) + one(left[1], right[0]))


def row_index(shape):
    return lax.broadcasted_iota(jnp.int32, shape, 0)


def lane_index(shape):
    return lax.broadcasted_iota(jnp.int32, shape, 1)


def row_after(block, last):
    rows = block.shape[0]
    moved = pltpu.roll(block, rows - 1, 0)
    return jnp.where(row_index(block.shape) == rows - 1, last, moved)


def row_before(block, first):
    moved = pltpu.roll(block, 1, 0)
    return jnp.where(row_index(block.shape) == 0, first, moved)


def lane_difference(block):
    lanes = block.shape[1]
    return pltpu.roll(block, lanes - 1, 1) - pltpu.roll(block, 1, 1)


def run_kernel(body, outs, args, scalars=(), scratch=(), flops=0, far=(), far_outs=(), aliases=None):
    outs = list(outs) if isinstance(outs, list) else outs
    leaves = list(args) + jax.tree.leaves(outs)
    leaves += [leaf for leaf in scratch if leaf.memory_space == pltpu.VMEM]
    held = sum(math.prod(leaf.shape) * jnp.dtype(leaf.dtype).itemsize for leaf in leaves)
    args = [
        pltpu.with_memory_space_constraint(arg, pltpu.HBM) if number in far else arg
        for number, arg in enumerate(args)
    ]
    spaces = jax.tree.map(lambda _: pl.BlockSpec(memory_space=pltpu.VMEM), outs)
    for number in far_outs:
        spaces[number] = pl.BlockSpec(memory_space=pltpu.HBM)
        outs[number] = pltpu.HBM(outs[number].shape, outs[number].dtype)
    in_specs = [pl.BlockSpec(memory_space=pltpu.SMEM) for _ in scalars]
    in_specs += [
        pl.BlockSpec(memory_space=pltpu.HBM if number in far else pltpu.VMEM)
        for number in range(len(args))
    ]
    return pl.pallas_call(
        body,
        out_shape=outs,
        in_specs=in_specs,
        out_specs=spaces,
        scratch_shapes=scratch,
        input_output_aliases=aliases or {},
        compiler_params=pltpu.CompilerParams(vmem_limit_bytes=held + (4 << 20)),
        cost_estimate=pl.CostEstimate(flops=flops, bytes_accessed=held, transcendentals=0),
    )(*scalars, *args)


def rim_rows(members):
    return -(-(6 * members + 18) // ROW_TILE) * ROW_TILE


def pack_rows(fields, flow, grp_index, groups):
    members, dims, size_x, size_y = fields.shape
    rows = size_x // groups
    planes = members * dims
    rim = rim_rows(members)
    shape = jax.ShapeDtypeStruct((planes * rows + rim, size_y), fields.dtype)

    def pack(index, source, motion, *refs):
        targets, singles = refs[:groups], refs[groups : groups + dims]
        held, ends, rims, fetched, ended, copied, alone, placed = refs[groups + dims :]
        last = motion.shape[1] - END_ROWS
        tips = [
            pltpu.make_async_copy(
                motion.at[:, first : first + END_ROWS, :], ends.at[side], ended.at[side]
            )
            for side, first in enumerate((0, last))
        ]
        loads = [
            pltpu.make_async_copy(source.at[:, dim], held.at[dim], fetched.at[dim])
            for dim in range(dims)
        ]
        for move in loads + tips:
            move.start()
        blocks = [(index[0] + shift) % groups for shift in range(groups)]
        moves = []
        for dim in range(dims):
            loads[dim].wait()
            for shift in range(1, groups):
                start = pl.multiple_of(blocks[shift] * rows, rows)
                for member in range(members):
                    plane = member * dims + dim
                    moves.append(
                        pltpu.make_async_copy(
                            held.at[dim, member, pl.ds(start, rows), :],
                            targets[shift].at[plane * rows : (plane + 1) * rows, :],
                            copied.at[shift, plane],
                        )
                    )
                    moves[-1].start()
            moves.append(pltpu.make_async_copy(held.at[dim], singles[dim], alone.at[dim]))
            moves[-1].start()
        start = pl.multiple_of(blocks[0] * rows, rows)
        for dim in range(dims):
            for member in range(members):
                plane = member * dims + dim
                targets[0][plane * rows : (plane + 1) * rows, :] = held[
                    dim, member, pl.ds(start, rows), :
                ]
        for move in tips:
            move.wait()
        place = row_index((rim, size_y))
        common = jnp.zeros((rim, size_y), jnp.float32)
        slot = 2 * planes
        for side, line in enumerate((0, END_ROWS - 1)):
            for dim in range(dims):
                rest = ends[side, dim][line : line + 1, :]
                for _ in range(3):
                    part = rest.astype(jnp.bfloat16).astype(jnp.float32)
                    rest = rest - part
                    common = jnp.where(place == slot, part, common)
                    slot += 1
        for shift in range(groups):
            above = pl.multiple_of(
                (blocks[shift] + groups - 1) % groups * rows + rows - ROW_TILE, ROW_TILE
            )
            below = pl.multiple_of((blocks[shift] + 1) % groups * rows, rows)
            edge = common
            for member in range(members):
                for dim in range(dims):
                    top = held[dim, member, pl.ds(above, ROW_TILE), :].astype(jnp.float32)
                    bottom = held[dim, member, pl.ds(below, ROW_TILE), :].astype(jnp.float32)
                    slot = dim * 2 * members + member * 2
                    edge = jnp.where(place == slot, top[ROW_TILE - 1 :], edge)
                    edge = jnp.where(place == slot + 1, bottom[:1], edge)
            if shift == 0:
                targets[0][planes * rows :, :] = edge.astype(fields.dtype)
                continue
            rims[shift] = edge.astype(fields.dtype)
            moves.append(
                pltpu.make_async_copy(
                    rims.at[shift],
                    targets[shift].at[planes * rows : planes * rows + rim, :],
                    placed.at[shift],
                )
            )
            moves[-1].start()
        for move in moves:
            move.wait()

    count = groups + dims
    return run_kernel(
        pack,
        [shape] * groups
        + [jax.ShapeDtypeStruct((members, size_x, size_y), fields.dtype)] * dims,
        [fields, flow],
        [grp_index],
        scratch=[
            pltpu.VMEM((dims, members, size_x, size_y), fields.dtype),
            pltpu.VMEM((2, 3, END_ROWS, size_y), flow.dtype),
            pltpu.VMEM((groups, rim, size_y), fields.dtype),
            pltpu.SemaphoreType.DMA((dims,)),
            pltpu.SemaphoreType.DMA((2,)),
            pltpu.SemaphoreType.DMA((groups, planes)),
            pltpu.SemaphoreType.DMA((dims,)),
            pltpu.SemaphoreType.DMA((groups,)),
        ],
        far=(0, 1),
        far_outs=range(1, count),
    )


def force_rows(blocks, motion, near, far, sign, table, members, field_total):
    rows, size_y = motion.shape[1:]
    planes = 3 * members
    rim = rim_rows(members)

    def stress_of(sums):
        stretch = stretch_factor((sums[0] + sums[1] + sums[2]) / field_total)
        return stretch, [
            POLY_MODULUS * (stretch * sums[slot] / field_total - (1.0 if first == second else 0.0))
            for slot, (first, second) in enumerate(TENSOR_PAIRS)
        ]

    def force(signs, *refs):
        parts = refs[: len(blocks)]
        flow, pair, other, tables, out, late, stress, stack = refs[len(blocks) :]
        side = signs[0].astype(jnp.float32)
        for start in range(0, rows, ROW_TILE):
            sums = [None] * 6
            for part in parts:
                for member in range(members):
                    vector = [
                        part[(member * 3 + dim) * rows + start :][:ROW_TILE, :].astype(jnp.float32)
                        if False
                        else part[
                            (member * 3 + dim) * rows + start : (member * 3 + dim) * rows
                            + start
                            + ROW_TILE,
                            :,
                        ].astype(jnp.float32)
                        for dim in range(3)
                    ]
                    for slot, (first, second) in enumerate(TENSOR_PAIRS):
                        term = vector[first] * vector[second]
                        sums[slot] = term if sums[slot] is None else sums[slot] + term
            stretch, values = stress_of(sums)
            late[3, start : start + ROW_TILE, :] = stretch
            for slot in range(6):
                stress[slot, start : start + ROW_TILE, :] = values[slot]
        sums = [None] * 6
        lines = []
        for part in parts:
            edge = part[planes * rows : planes * rows + rim, :].astype(jnp.float32)
            lines.append(edge[2 * planes :])
            vector = [edge[dim * 2 * members : (dim + 1) * 2 * members] for dim in range(3)]
            for slot, (first, second) in enumerate(TENSOR_PAIRS):
                term = vector[first] * vector[second]
                sums[slot] = term if sums[slot] is None else sums[slot] + term
        sums = [
            sum(value[2 * member : 2 * member + 2] for member in range(members)) for value in sums
        ]
        edges = stress_of(sums)[1]
        bottom = [sum(lines[-1][3 * c + t : 3 * c + t + 1] for t in range(3)) for c in range(3)]
        top = [sum(lines[1][9 + 3 * c + t : 10 + 3 * c + t] for t in range(3)) for c in range(3)]
        half = 0.5 * TIME_STEP
        place = {0: 0, 1: 1, 2: 4}
        for component in range(3):
            slot_x = pair_slot(component, 0)
            slot_y = pair_slot(component, 1)
            slot_z = pair_slot(component, 2)
            value = stress[slot_x]
            total = row_after(value, edges[slot_x][1:2]) - row_before(value, edges[slot_x][0:1])
            total = total + lane_difference(stress[slot_y])
            own = flow[component]
            total = total - flow[0] * (
                row_after(own, bottom[component]) - row_before(own, top[component])
            )
            total = total - flow[1] * lane_difference(own)
            rise = side * (pair[component] - other[component])
            late[component] = 0.5 * rise
            total = total - flow[2] * rise
            spot = place[component]
            stack[spot * rows : (spot + 1) * rows, :] = own + half * total
            spot = spot + (2 if component < 2 else 1)
            stack[spot * rows : (spot + 1) * rows, :] = half * stress[slot_z]
        out[...] = dot_split((tables[0], tables[1]), split_value(stack[...]), ((1,), (1,)))

    return run_kernel(
        force,
        [
            jax.ShapeDtypeStruct((size_y, 6 * rows), jnp.float32),
            jax.ShapeDtypeStruct((4, rows, size_y), jnp.float32),
        ],
        [*blocks, motion, near, far, table],
        [sign],
        scratch=[
            pltpu.VMEM((6, rows, size_y), jnp.float32),
            pltpu.VMEM((6 * rows, size_y), jnp.float32),
        ],
    )


def solve_pencil(pencil, device_index, table, groups, total_z, size_y):
    block = pencil.shape[1]
    pairs = block // 2
    rows = pencil.shape[2] // 6
    size_x = rows * groups
    half_x = size_x // 2
    half_z = total_z // 2
    basis_z = real_basis(total_z)
    lines = total_z * block
    step_x = 2.0 * math.pi / size_x
    step_y = 2.0 * math.pi / size_y
    step_z = 2.0 * math.pi / total_z

    def join(first, second, lane):
        return jnp.where(lane < rows, first, pltpu.roll(second, rows, 1))

    def solve(index, source, tables, out, stack, result):
        lane = lane_index((block, 2 * rows))
        for pair in range(groups // 2):
            both = []
            for side in range(2):
                group = 2 * pair + side
                tiles = [
                    [
                        source[group * total_z + z, :, t * 2 * rows : (t + 1) * 2 * rows]
                        for t in range(3)
                    ]
                    for z in range(total_z)
                ]
                both.append(
                    [
                        (
                            tiles[z][0] + tiles[(z + 1) % total_z][1] - tiles[z - 1][1],
                            tiles[z][2]
                            + pltpu.roll(tiles[(z + 1) % total_z][2] - tiles[z - 1][2], rows, 1),
                        )
                        for z in range(total_z)
                    ]
                )
            columns = slice(pair * 2 * rows, (pair + 1) * 2 * rows)
            for z in range(total_z):
                (first, third), (first_b, third_b) = both[0][z], both[1][z]
                line = z * block
                stack[line : line + block, columns] = join(first, first_b, lane)
                stack[lines + line : lines + line + block, columns] = jnp.where(
                    lane < rows, pltpu.roll(first, rows, 1), first_b
                )
                stack[2 * lines + line : 2 * lines + line + block, columns] = join(
                    third, third_b, lane
                )
        table_x = (tables[2], tables[3])
        result[...] = dot_split(split_value(stack[...]), table_x, ((1,), (0,)))

        shape = (block, size_x)
        lane = lane_index(shape)
        row = row_index(shape)
        wave = (lane % half_x).astype(jnp.float32) * step_x
        nyquist_x = jnp.where(lane == half_x, math.pi, 0.0)
        swap_x = jnp.where(lane < half_x, wave, -wave)
        square_x = wave * wave + nyquist_x * nyquist_x
        weight_x = jnp.where(lane % half_x == 0, 1.0, 2.0)
        number = index[0] * pairs + row % pairs
        wave = number.astype(jnp.float32) * step_y
        nyquist_y = jnp.where((number == 0) & (row >= pairs), math.pi, 0.0)
        swap_y = jnp.where(row < pairs, wave, -wave)
        square_y = wave * wave + nyquist_y * nyquist_y
        weight_y = jnp.where(number == 0, 1.0, 2.0)
        square_xy = square_x + square_y
        scale = weight_x * weight_y / (size_x * size_y * total_z)

        def along_x(value):
            return swap_x * pltpu.roll(value, half_x, 1)

        def along_y(value):
            return swap_y * pltpu.roll(value, pairs, 0)

        waves = []
        for component in range(3):
            planes = [
                result[component * lines + z * block : component * lines + (z + 1) * block, :]
                for z in range(total_z)
            ]
            waves.append(
                [
                    sum(float(basis_z[z, k]) * planes[z] for z in range(total_z))
                    for k in range(total_z)
                ]
            )

        def partner(k):
            if k % half_z == 0:
                return k, 0.0
            return (k + half_z, step_z * k) if k < half_z else (k - half_z, -step_z * (k - half_z))

        potential = []
        factors = []
        extra = []
        for k in range(total_z):
            wave_z = step_z * (k % half_z) if k != half_z else math.pi
            square = square_xy + wave_z * wave_z
            safe = jnp.where(square > 0, square, 1.0)
            other, factor = partner(k)
            total = along_x(waves[0][k]) + along_y(waves[1][k])
            if factor != 0.0:
                total = total + factor * waves[2][other]
            potential.append(total / safe)
            nyquist = nyquist_x * waves[0][k] + nyquist_y * waves[1][k]
            if k == half_z:
                nyquist = nyquist + math.pi * waves[2][k]
            extra.append(nyquist / safe)
            weight_z = 1.0 if k % half_z == 0 else 2.0
            factors.append(scale * weight_z / (1.0 + VISCOSITY * TIME_STEP * square))
        solved = [[], [], []]
        for k in range(total_z):
            other, factor = partner(k)
            solved[0].append(
                factors[k] * (waves[0][k] + along_x(potential[k]) - nyquist_x * extra[k])
            )
            solved[1].append(
                factors[k] * (waves[1][k] + along_y(potential[k]) - nyquist_y * extra[k])
            )
            value = waves[2][k]
            if factor != 0.0:
                value = value + factor * potential[other]
            if k == half_z:
                value = value - math.pi * extra[k]
            solved[2].append(factors[k] * value)
        for component in range(3):
            for z in range(total_z):
                line = component * lines + z * block
                stack[line : line + block, :] = sum(
                    float(basis_z[z, k]) * solved[component][k] for k in range(total_z)
                )
        result[...] = dot_split(split_value(stack[...]), table_x, ((1,), (1,)))
        lane = lane_index((block, 2 * rows))
        for group in range(groups):
            columns = slice(group // 2 * 2 * rows, (group // 2 + 1) * 2 * rows)
            for z in range(total_z):
                line = z * block
                held = [
                    result[c * lines + line : c * lines + line + block, columns] for c in range(3)
                ]
                turned = [pltpu.roll(value, rows, 1) for value in held]
                low, high = (held, turned) if group % 2 == 0 else (turned, held)
                tiles = (
                    jnp.where(lane < rows, low[0], high[1]),
                    jnp.where(lane < rows, low[2], pltpu.roll(high[0], pairs, 0)),
                    pltpu.roll(jnp.where(lane < rows, low[1], high[2]), pairs, 0),
                )
                for number, tile in enumerate(tiles):
                    spot = slice(number * 2 * rows, (number + 1) * 2 * rows)
                    out[group * total_z + z, :, spot] = tile[:pairs]

    return run_kernel(
        solve,
        jax.ShapeDtypeStruct((groups * total_z, pairs, 6 * rows), jnp.float32),
        [pencil, table],
        [device_index],
        scratch=[
            pltpu.VMEM((3 * lines, size_x), jnp.float32),
            pltpu.VMEM((3 * lines, size_x), jnp.float32),
        ],
    )


def rows_from_waves(spectra, table, rows):
    devices, pairs, lanes = spectra.shape
    size_y = table.shape[2]
    joined = max(8 // pairs, 1)

    def synthesise(source, tables, out, stack):
        for first in range(0, devices, joined):
            blocks = [source[device] for device in range(first, first + joined)]
            stack[first * pairs : (first + joined) * pairs, :] = jnp.concatenate(blocks, axis=0)
        turned = stack[...].T
        waves = jnp.concatenate([turned[: 3 * rows], turned[3 * rows :]], axis=1)
        value = dot_split(split_value(waves), (tables[2], tables[3]), ((1,), (1,)))
        for component in range(3):
            out[component, 0] = value[component * rows : (component + 1) * rows]

    return run_kernel(
        synthesise,
        jax.ShapeDtypeStruct((3, 1, rows, size_y), jnp.float32),
        [spectra, table],
        scratch=[pltpu.VMEM((devices * pairs, lanes), jnp.float32)],
    )


def advance_fields(fields, near, far, motions, lates, noise, grp_index, offsets, sign):
    members, _, size_x, size_y = fields.shape
    count = len(offsets)
    rows = size_x // count
    steps = size_x // ROW_TILE
    half = 0.5 * TIME_STEP

    def advance(spot, signs, kick, own, *refs):
        close, remote, refs = refs[:2], refs[2:4], refs[4:]
        flows, others, refs = refs[:count], refs[count : 2 * count], refs[2 * count :]
        out, rest, pace, plane, ready, sent = refs
        for number in range(count):
            start = pl.multiple_of((spot[0] ^ offsets[number]) * rows, rows)
            for slot in range(3):
                plane[slot, pl.ds(start, rows), :] = flows[number][slot]
            for slot in range(4):
                plane[3 + slot, pl.ds(start, rows), :] = others[number][slot]
        side = signs[0].astype(jnp.float32)

        def step(number, carry):
            start = pl.multiple_of(number * ROW_TILE, ROW_TILE)
            before = pl.multiple_of((number + steps - 1) % steps * ROW_TILE, ROW_TILE)
            after = pl.multiple_of((number + 1) % steps * ROW_TILE, ROW_TILE)
            here = pl.ds(start, ROW_TILE)
            speed = [half * plane[c, here, :] for c in range(3)]
            slope = []
            for c in range(3):
                first = half * plane[c, pl.ds(before, ROW_TILE), :][ROW_TILE - 1 :]
                last = half * plane[c, pl.ds(after, ROW_TILE), :][:1]
                slope.append(
                    (
                        row_after(speed[c], last) - row_before(speed[c], first),
                        lane_difference(speed[c]),
                        TIME_STEP * plane[3 + c, here, :],
                    )
                )
            keep = 1.0 - (TIME_STEP / (2.0 * RELAX_TIME)) * plane[6, here, :]
            lift = side * speed[2]
            pace[here, :] = lift
            for member in range(members):
                vector = [own[member, c, here, :].astype(jnp.float32) for c in range(3)]
                for c in range(3):
                    first = own[member, c, pl.ds(before, ROW_TILE), :].astype(jnp.float32)
                    last = own[member, c, pl.ds(after, ROW_TILE), :].astype(jnp.float32)
                    value = vector[c]
                    total = keep * value + NOISE_SCALE * kick[member, c]
                    for j in range(3):
                        total = total + slope[c][j] * vector[j]
                    total = total - speed[0] * (
                        row_after(value, last[:1]) - row_before(value, first[ROW_TILE - 1 :])
                    )
                    total = total - speed[1] * lane_difference(value)
                    if c == 2:
                        rest[member, here, :] = total
                        continue
                    rise = close[c][member, here, :].astype(jnp.float32)
                    rise = rise - remote[c][member, here, :].astype(jnp.float32)
                    ready[c, member, here, :] = (total - lift * rise).astype(ready.dtype)
            return carry

        lax.fori_loop(0, steps, step, 0)
        moves = [
            pltpu.make_async_copy(ready.at[c], out.at[:, c], sent.at[c]) for c in range(2)
        ]
        for move in moves:
            move.start()
        for move in moves:
            move.wait()

    return run_kernel(
        advance,
        [
            jax.ShapeDtypeStruct(fields.shape, fields.dtype),
            jax.ShapeDtypeStruct((members, size_x, size_y), jnp.float32),
            jax.ShapeDtypeStruct((size_x, size_y), jnp.float32),
        ],
        [fields, *near, *far, *motions, *lates],
        [grp_index, sign, noise],
        scratch=[
            pltpu.VMEM((7, size_x, size_y), jnp.float32),
            pltpu.VMEM((2, members, size_x, size_y), fields.dtype),
            pltpu.SemaphoreType.DMA((2,)),
        ],
        far_outs=(0,),
        flops=200 * members * size_x * size_y,
    )


def finish_fields(fields, rest, pace, near, far):
    members, size_x, size_y = rest.shape

    def finish(partial, speed, close, remote, _, out, ready, sent):
        for member in range(members):
            rise = close[member].astype(jnp.float32) - remote[member].astype(jnp.float32)
            ready[member] = (partial[member] - speed[...] * rise).astype(ready.dtype)
        move = pltpu.make_async_copy(ready, out.at[:, 2], sent)
        move.start()
        move.wait()

    return run_kernel(
        finish,
        [jax.ShapeDtypeStruct(fields.shape, fields.dtype)],
        [rest, pace, near, far, fields],
        scratch=[
            pltpu.VMEM((members, size_x, size_y), fields.dtype),
            pltpu.SemaphoreType.DMA(()),
        ],
        flops=4 * members * size_x * size_y,
        far=(4,),
        far_outs=(0,),
        aliases={4: 0},
    )[0]


def shifted(value, axis, step):
    count = lax.axis_size(axis)
    return lax.ppermute(value, axis, [(i, (i + step) % count) for i in range(count)])


def flipped(value, axis, bit):
    count = lax.axis_size(axis)
    return lax.ppermute(value, axis, [(i, i ^ bit) for i in range(count)])


def spread(value, axis):
    bit = lax.axis_size(axis) // 2
    found = [(0, value)]
    while bit:
        for offset, held in list(found):
            found.append((offset ^ bit, flipped(held, axis, bit)))
        bit //= 2
    return found


def pencil_shards(velocity, fields, noise):
    groups = lax.axis_size("grp")
    slabs = lax.axis_size("slab")
    grp_index = lax.axis_index("grp")
    slab_index = lax.axis_index("slab")
    members, _, _, size_x, size_y = fields.shape
    rows = velocity.shape[2]
    devices = groups * slabs
    block = size_y // devices
    half_block = block // 2
    order = np.concatenate(
        [
            np.concatenate([np.arange(half_block), size_y // 2 + np.arange(half_block)])
            + device * half_block
            for device in range(devices)
        ]
    )
    table = split_tables(np.ascontiguousarray(real_basis(size_y).T[order]), real_basis(size_x))

    flow = velocity[:, 0]
    plane = fields[:, :, 0]
    two_up = [(i, (i + (-2 if i % 2 else 2)) % slabs) for i in range(slabs)]
    sign = (1 - 2 * (slab_index & 1)).reshape(1)
    packed = pack_rows(plane, flow, grp_index.reshape(1), groups)
    blocks, parts = packed[:groups], packed[groups:]
    received = [blocks[0]]
    for d in range(1, groups):
        received.append(shifted(blocks[d], "grp", d))
    flow_near = flipped(flow, "slab", 1)
    flow_far = lax.ppermute(flow_near, "slab", two_up)
    two_down = [(target, source) for source, target in two_up]
    near = []
    for part in parts:
        near.append(flipped(part, "slab", 1))
    hopped = lax.ppermute(parts[0], "slab", two_down)
    far = [flipped(hopped, "slab", 1)]
    far.append(lax.ppermute(near[1], "slab", two_up))
    motions = spread(flow, "grp")
    spectra, late = force_rows(
        received, flow, flow_near, flow_far, sign, table, members, members * groups
    )
    lates = spread(late, "grp")
    pencil = lax.all_to_all(
        spectra.reshape(devices, block, 6 * rows),
        ("grp", "slab"),
        split_axis=0,
        concat_axis=0,
        tiled=True,
    )
    last, pencil = lax.optimization_barrier((near[2], pencil))
    far.append(lax.ppermute(last, "slab", two_up))
    device_index = (grp_index * slabs + slab_index).reshape(1)
    solved = solve_pencil(pencil, device_index, table, groups, slabs, size_y)
    new_fields, rest, pace = advance_fields(
        plane,
        near[:2],
        far[:2],
        [held for _, held in motions],
        [held for _, held in lates],
        noise,
        grp_index.reshape(1),
        [offset for offset, _ in motions],
        sign,
    )
    new_fields = finish_fields(new_fields, rest, pace, near[2], far[2])
    solved = lax.all_to_all(
        solved, ("grp", "slab"), split_axis=0, concat_axis=0, tiled=True
    )
    new_velocity = rows_from_waves(solved, table, rows)
    return (new_velocity, new_fields[:, :, None])


def pencil_fits(mesh, velocity, fields):
    groups, slabs = mesh.shape["grp"], mesh.shape["slab"]
    size_z, size_x, size_y = velocity.shape[1:]
    return (
        size_z == slabs
        and size_x == size_y
        and slabs % 2 == 0
        and groups >= 2
        and groups & (groups - 1) == 0
        and size_y % (2 * groups * slabs) == 0
        and size_x % (groups * ROW_TILE) == 0
        and (2 * size_x // groups) % 128 == 0
        and fields.shape[0] % groups == 0
    )


def solution(mesh):
    specs = (P(None, "slab", "grp", None), P("grp", None, "slab", None, None), P("grp", None))

    def mapped(body):
        return jax.shard_map(body, mesh=mesh, in_specs=specs, out_specs=specs[:2], check_vma=False)

    def step(velocity, fields, noise):
        if not pencil_fits(mesh, velocity, fields):
            return mapped(shards)(velocity, fields, noise)
        return mapped(pencil_shards)(velocity, fields, noise)

    return step
```
